128 devices in a mesh: tmpl: 2 (over core), row: 16 (over y, z), col: 4 (over x).
Axes of the slice: x: 4, y: 4, z: 4, core: 2. Of those that a mesh axis runs over, the one named last changes fastest.
Arguments:
- template_pair: bfloat16 [2, 512, 64, 512], P('tmpl', 'row', None, 'col'), may hold values from -6 to 6
- trunk: bfloat16 [512, 128, 512], P('row', None, 'col'), may hold values from -6 to 6
- coverage: int32 [2, 512], replicated, may hold values from 0 to 1, as said below
- chain_ids: int32 [512], replicated, may hold values from 0 to 3, never falling along the last dimension, each value on 1 to 256 neighbouring positions
- chain_vec: float32 [64], replicated, may hold values from -4 to 4
- trunk_weights: bfloat16 [64, 128], replicated, may hold values from -0.5 to 0.5
- proj_weights: bfloat16 [2, 5, 64, 64], replicated, may hold values from -0.75 to 0.75
- out_weights: bfloat16 [2, 64, 64], replicated, may hold values from -0.75 to 0.75
- final_weights: bfloat16 [128, 64], replicated, may hold values from -0.75 to 0.75
Outputs:
- trunk_out: bfloat16 [512, 128, 512], P('row', None, 'col')
The draws below stay inside these ranges and needn't reach their ends.
Inputs may be any that keep to these rules, and one draw needn't show every extreme that they name: coverage[t, i] is 1 where template t covers token i, else 0; how densely a template covers tokens is drawn anew for each block of 32 consecutive tokens. `chain_ids`: chain ids never fall along the tokens.
All inputs are finite; a program needn't handle non-finite values.
Results may differ from the reference program's by a relative error of at most 0.008.
Values may be sent and summed in bfloat16 or wider, within the bound.
A program may use at most 128 MiB of HBM per device.

```python
import math
import jax
import jax.numpy as jnp
import numpy as np
from jax import lax

C = 64
CZ = 128
N = 512
TEMPLATES = 2
ROWS = 32
COLS = 128
N_ROW = 16
N_COL = 4


def draw_coverage(key, part):
    level_key = jax.random.fold_in(key, 11)
    coin_key = jax.random.fold_in(key, 23)
    levels = jax.random.randint(level_key, (TEMPLATES, N // ROWS), 0, 4)
    spread_levels = jnp.repeat(levels, ROWS, axis=1)
    coins = jax.random.randint(coin_key, (TEMPLATES, N), 0, 4)
    return (coins < spread_levels).astype(jnp.int32)


def level_of(key, extent, cuts, smallest, high):
    factor_of, own = 1.0, jax.random.fold_in(key, 6)
    for position, parts in cuts:
        draws = jnp.exp(jax.random.uniform(jax.random.fold_in(own, position), (parts,), jnp.float32, smallest / len(cuts), high / len(cuts)))
        factor_of = factor_of * jnp.repeat(draws, extent[position] // parts).reshape([-1 if axis == position else 1 for axis in range(len(extent))])
    return factor_of


def profile(number_of, total, most, skew):
    loads = [(1 << 20) // math.isqrt(grade ** skew) + 1 for grade in range(2, number_of + 1)]
    rest, holding = total - most - (number_of - 1), [1] * (number_of - 1)
    while rest > 0:
        candidates = [i for i in range(number_of - 1) if holding[i] < most]
        mass, budget = sum([loads[i] for i in candidates]), rest
        for i in candidates:
            more = min(most - holding[i], max(1, budget * loads[i] // mass), rest)
            holding[i] = holding[i] + more
            rest = rest - more
    return np.array([most] + holding)


def ragged(key, amount, total, most, skew):
    if amount == 2:
        one = jax.random.randint(key, (), max(1, total - most), min(most, total - 1) + 1)
        return jnp.stack([one, total - one])
    sizes = jnp.asarray(profile(amount, total, most, skew), jnp.int32)
    couples = (amount - 1) // 2
    source_of, sink = sizes[1:1 + 2 * couples:2], sizes[2:2 + 2 * couples:2]
    room = jnp.minimum(source_of - 1, most - sink)
    shifted = jax.random.randint(jax.random.fold_in(key, 1), (couples,), 0, 1 << 20) % (room + 1)
    sizes = sizes.at[1:1 + 2 * couples:2].set(source_of - shifted).at[2:2 + 2 * couples:2].set(sink + shifted)
    return sizes[jax.random.permutation(jax.random.fold_in(key, 2), amount)]


def gaussian(stream_key, extent, deviation, most, split=(), dtype=jnp.bfloat16):
    result = deviation * jax.random.normal(stream_key, extent, jnp.float32)
    if split:
        result = result * level_of(stream_key, extent, split, -0.22, 0.18)
    return jnp.clip(result, -most, most).astype(dtype)


def setup_inputs(seed: int = 0) -> dict:
    splits = jax.random.split(jax.random.key(seed), 10)
    template_pair = gaussian(splits[0], (TEMPLATES, N, C, N), 1.0, 6.0, ((0, 2), (1, 16), (3, 4)))
    trunk = gaussian(splits[1], (N, CZ, N), 1.0, 6.0, ((0, 16), (2, 4)))
    coverage = draw_coverage(jax.random.fold_in(splits[9], 71), 0)
    chain_ids = jnp.searchsorted(jnp.cumsum(ragged(splits[3], 4, N, N // 2, 2)), jnp.arange(N), side="right").astype(jnp.int32)
    chain_vec = gaussian(splits[4], (C,), 1.0, 4.0, (), jnp.float32)
    trunk_weights = gaussian(splits[5], (C, CZ), CZ ** -0.5, 0.5)
    proj_weights = gaussian(splits[6], (2, 5, C, C), C ** -0.5, 0.75)
    out_weights = gaussian(splits[7], (2, C, C), C ** -0.5, 0.75)
    final_weights = gaussian(splits[8], (CZ, C), C ** -0.5, 0.75)
    return {"template_pair": template_pair, "trunk": trunk, "coverage": coverage, "chain_ids": chain_ids, "chain_vec": chain_vec, "trunk_weights": trunk_weights, "proj_weights": proj_weights, "out_weights": out_weights, "final_weights": final_weights}


epsilon = 1e-05

def channel_norm(values):
    centre = lax.optimization_barrier(jnp.mean(values, axis=1, keepdims=True))
    centred = values - centre
    spread = lax.optimization_barrier(jnp.mean(centred * centred, axis=1, keepdims=True))
    return centred * lax.rsqrt(spread + epsilon)

def project(weights, values):
    return jnp.einsum('dc,icj->idj', weights.astype(jnp.float32), values.astype(jnp.float32))

def rounded(values):
    return lax.optimization_barrier(values.astype(jnp.bfloat16)).astype(jnp.float32)

def gated_pair(pair_rep, pair_mask, weights):
    normed = channel_norm(pair_rep.astype(jnp.float32)).astype(jnp.bfloat16)
    pieces = [project(weights[number], normed) for number in range(5)]
    weighted = pair_mask[:, None, :]
    left_proj = (weighted * jax.nn.sigmoid(pieces[0]) * pieces[1]).astype(jnp.bfloat16)
    right_proj = (weighted * jax.nn.sigmoid(pieces[2]) * pieces[3]).astype(jnp.bfloat16)
    return (left_proj, right_proj, pieces[4])

def apply_update(pair_rep, tri_sum, gate_proj, weights):
    tri_norm = channel_norm(tri_sum).astype(jnp.bfloat16)
    update = jax.nn.sigmoid(gate_proj) * project(weights, tri_norm)
    return (pair_rep.astype(jnp.float32) + update).astype(jnp.bfloat16)

def outgoing_sum(left_proj, right_proj):
    tri_sum = jnp.zeros((N, left_proj.shape[1], N), jnp.float32)
    for block_number in range(N_COL):
        lower = block_number * COLS
        left_block = left_proj[:, :, lower:lower + COLS].astype(jnp.float32)
        right_block = right_proj[:, :, lower:lower + COLS].astype(jnp.float32)
        tri_sum = tri_sum + rounded(jnp.einsum('ick,jck->icj', left_block, right_block))
    return tri_sum

def incoming_sum(left_proj, right_proj):
    tri_sum = jnp.zeros((N, left_proj.shape[1], N), jnp.float32)
    for block_number in range(N_ROW):
        lower = block_number * ROWS
        left_block = left_proj[lower:lower + ROWS].astype(jnp.float32)
        right_block = right_proj[lower:lower + ROWS].astype(jnp.float32)
        tri_sum = tri_sum + rounded(jnp.einsum('kci,kcj->icj', left_block, right_block))
    return tri_sum

def reference(template_pair, trunk, coverage, chain_ids, chain_vec, trunk_weights, proj_weights, out_weights, final_weights):
    same_chain = (chain_ids[:, None] == chain_ids[None, :]).astype(jnp.float32)
    cover_float = coverage.astype(jnp.float32)
    cover_count = lax.optimization_barrier(jnp.sum(cover_float[:, :, None] * cover_float[:, None, :], axis=0))
    trunk_proj = project(trunk_weights, channel_norm(trunk.astype(jnp.float32)))
    pooled = jnp.zeros((N, template_pair.shape[2], N), jnp.float32)
    for template_index in range(TEMPLATES):
        pair_mask = cover_float[template_index][:, None] * cover_float[template_index][None, :]
        pair_rep = (template_pair[template_index].astype(jnp.float32) + same_chain[:, None, :] * chain_vec[None, :, None] + trunk_proj).astype(jnp.bfloat16)
        left_proj, right_proj, gate_proj = gated_pair(pair_rep, pair_mask, proj_weights[0])
        pair_rep = apply_update(pair_rep, outgoing_sum(left_proj, right_proj), gate_proj, out_weights[0])
        left_proj, right_proj, gate_proj = gated_pair(pair_rep, pair_mask, proj_weights[1])
        pair_rep = apply_update(pair_rep, incoming_sum(left_proj, right_proj), gate_proj, out_weights[1])
        pooled = pooled + pair_mask[:, None, :] * channel_norm(pair_rep.astype(jnp.float32))
    hidden = jax.nn.relu(pooled / jnp.maximum(cover_count, 1.0)[:, None, :]).astype(jnp.bfloat16)
    return (trunk.astype(jnp.float32) + project(final_weights, hidden)).astype(jnp.bfloat16)
```

```python
import functools

import jax
import jax.numpy as jnp
from jax import lax
from jax.experimental import pallas as pl
from jax.experimental.pallas import tpu as pltpu
from jax.sharding import PartitionSpec as P

MESH = pl.DeviceIdType.MESH
EPS = 1e-05
F32 = jnp.float32
BF16 = jnp.bfloat16
ROWS, COLS, C, CZ = 32, 128, 64, 128
HALF = 16
DEV = 64


def dot(a, b):
    return jnp.dot(a, b, preferred_element_type=F32)


def iota(shape, dim):
    return lax.broadcasted_iota(jnp.int32, shape, dim)


def to_rhs(x):
    a = x[:, 0:8].reshape(512, COLS).astype(BF16)
    b = x[:, 8:16].reshape(512, COLS).astype(BF16)
    return jnp.concatenate([a, b], axis=1)


def from_out(o):
    a = o[:, 0:COLS].reshape(C, 8, COLS)
    b = o[:, COLS:].reshape(C, 8, COLS)
    return jnp.concatenate([a, b], axis=1)


def norm0(x):
    centred = x - jnp.mean(x, axis=0, keepdims=True)
    spread = jnp.mean(centred * centred, axis=0, keepdims=True)
    return centred * lax.rsqrt(spread + EPS)


def sigmoid(x):
    return 0.5 * jnp.tanh(0.5 * x) + 0.5


def kron_rows():
    return (iota((512, C), 0) // 8 == iota((512, C), 1)).astype(BF16)


def kron_cols():
    return (iota((C, 512), 1) // 8 == iota((C, 512), 0)).astype(BF16)


def kron8(w):
    tall = dot(kron_rows(), w).astype(BF16)
    full = dot(tall, kron_cols())
    same = lax.rem(iota((512, 512), 0), 8) == lax.rem(iota((512, 512), 1), 8)
    return jnp.where(same, full, 0.0).astype(BF16)


def kernel(
    tp_hbm, trunk_hbm, cover_ref, chain_ref, vec_ref, wt_ref, wp_ref, wo_ref, wf_ref,
    out_hbm,
    tp_v, tr_v, out_v, k_perm, k_trunk, k_proj, k_out, k_final,
    pair_v, normed_v, gate_v, sbuf, rbuf, tsend, tbuf, psend, pbuf,
    ld_sem, st_sem, own_sem, ssem, rsem, tssem, trsem, pssem, prsem,
):
    tmpl = lax.axis_index("tmpl")
    row = lax.axis_index("row")
    x = lax.axis_index("col")
    y, z = lax.div(row, 4), lax.rem(row, 4)
    me = x * 16 + row

    load_tp = pltpu.make_async_copy(tp_hbm.at[0], tp_v, ld_sem.at[0])
    load_tr = pltpu.make_async_copy(trunk_hbm, tr_v, ld_sem.at[1])
    load_tp.start()
    load_tr.start()

    def peer(step):
        mixed = lax.rem(step * 29, DEV)
        px = lax.rem(x + lax.rem(mixed, 4), 4)
        py = lax.rem(y + lax.rem(lax.div(mixed, 4), 4), 4)
        pz = lax.rem(z + lax.div(mixed, 16), 4)
        prow = py * 4 + pz
        return prow, px, px * 16 + prow

    barrier = pltpu.get_barrier_semaphore()

    def greet(step, carry):
        prow, pcol, _ = peer(step)
        pl.semaphore_signal(
            barrier, inc=1, device_id=(tmpl, prow, pcol), device_id_type=MESH
        )
        return carry

    lax.fori_loop(1, DEV, greet, 0)
    pl.semaphore_signal(barrier, inc=1, device_id=(1 - tmpl, row, x), device_id_type=MESH)

    def send_all(source, target, send_sem, recv_sem):
        def send(step, carry):
            prow, pcol, number = peer(step)
            pltpu.make_async_remote_copy(
                src_ref=source(number), dst_ref=target, send_sem=send_sem, recv_sem=recv_sem,
                device_id=(tmpl, prow, pcol), device_id_type=MESH,
            ).start()
            return carry

        lax.fori_loop(1, DEV, send, 0)

    def wait_all(view, sem):
        pltpu.make_async_copy(view, view, sem).wait()

    def part(ref, number, h):
        return ref.at[number, :, pl.ds(h * HALF, HALF), :]

    cover = cover_ref[...].astype(F32)
    picks = (iota((ROWS, 512), 1) == row * ROWS + iota((ROWS, 512), 0)).astype(BF16)

    def row_plane(line):
        spread = jnp.broadcast_to(line, (COLS, 512)).astype(BF16)
        return lax.dot_general(picks, spread, (((1,), (1,)), ((), ())), preferred_element_type=F32)

    lanes = pl.ds(pl.multiple_of(x * COLS, COLS), COLS)
    cols_of = cover_ref[:, lanes].astype(F32)
    masks = [row_plane(cover[t : t + 1]) * cols_of[t : t + 1] for t in range(2)]
    mask = jnp.where(tmpl == 0, masks[0], masks[1])
    count = jnp.maximum(masks[0] + masks[1], 1.0)
    chain_rows = row_plane(chain_ref[...].astype(F32))
    same_chain = jnp.where(chain_rows == chain_ref[:, lanes].astype(F32), 1.0, 0.0)

    left_row, left_col = iota((512, 512), 0), iota((512, 512), 1)
    k_perm[...] = jnp.where(
        (lax.div(left_row, 8) == lax.rem(left_col, C)) & (lax.rem(left_row, 8) == lax.div(left_col, C)),
        1.0, 0.0,
    ).astype(BF16)
    tall_trunk = dot(kron_rows(), wt_ref[...])
    for i in range(8):
        keep = lax.rem(iota((512, CZ), 0), 8) == i
        k_trunk[:, i * CZ : (i + 1) * CZ] = jnp.where(keep, tall_trunk, 0.0).astype(BF16)
    for d in range(4):
        k_proj[0, d] = kron8(wp_ref[0, d])

    def products(m, h):
        rhs = normed_v[h]
        plane = mask[h * HALF : (h + 1) * HALF][None]
        for side in range(2):
            gate = from_out(dot(k_proj[m, 2 * side], rhs))
            value = from_out(dot(k_proj[m, 2 * side + 1], rhs))
            sbuf[m, :, side, h * HALF : (h + 1) * HALF, :] = (plane * sigmoid(gate) * value).astype(BF16)

    def gates(m, h):
        gate_v[h] = sigmoid(from_out(dot(k_proj[m, 4], normed_v[h])))

    def updated(m, h, tri):
        tri_norm = to_rhs(norm0(tri))
        update = gate_v[h] * from_out(dot(k_out[m], tri_norm))
        return (pair_v[h].astype(F32) + update).astype(BF16)

    load_tp.wait()
    load_tr.wait()
    for h in range(2):
        lo = h * HALF
        tr = tr_v[lo : lo + HALF].astype(F32)
        centred = tr - jnp.mean(tr, axis=1, keepdims=True)
        spread = jnp.mean(centred * centred, axis=1, keepdims=True)
        trn = (centred * lax.rsqrt(spread + EPS)).astype(BF16)
        rhs = jnp.concatenate(
            [trn[0:8].reshape(8 * CZ, COLS), trn[8:16].reshape(8 * CZ, COLS)], axis=1
        )
        pair = from_out(dot(k_trunk[...], rhs))
        tp = tp_v[lo : lo + HALF]
        rhs = jnp.concatenate([tp[0:8].reshape(512, COLS), tp[8:16].reshape(512, COLS)], axis=1)
        pair = pair + from_out(dot(k_perm[...], rhs))
        pair = pair + same_chain[lo : lo + HALF][None] * vec_ref[...]
        pair = pair.astype(BF16)
        pair_v[h] = pair
        normed_v[h] = to_rhs(norm0(pair.astype(F32)))
        products(0, h)
        if h == 0:
            pl.semaphore_wait(barrier, DEV)
        send_all(lambda n: part(sbuf.at[0], n, h), part(rbuf.at[0], me, h), ssem.at[0, h], rsem.at[0, h])
        pltpu.make_async_copy(part(sbuf.at[0], me, h), part(rbuf.at[0], me, h), own_sem.at[0, h]).start()

    k_proj[0, 4] = kron8(wp_ref[0, 4])
    for h in range(2):
        gates(0, h)
    for m in range(2):
        k_out[m] = kron8(wo_ref[m])
    for d in range(5):
        k_proj[1, d] = kron8(wp_ref[1, d])
    wide = dot(wf_ref[...], kron_cols())
    for i in range(8):
        keep = lax.rem(iota((CZ, 512), 1), 8) == i
        k_final[i * CZ : (i + 1) * CZ, :] = jnp.where(keep, wide, 0.0).astype(BF16)

    def wait_products(m):
        for h in range(2):
            view = rbuf.at[m, pl.ds(0, DEV - 1), :, pl.ds(h * HALF, HALF), :]
            wait_all(view, rsem.at[m, h])
            pltpu.make_async_copy(part(sbuf.at[m], me, h), part(rbuf.at[m], me, h), own_sem.at[m, h]).wait()

    def gathered(m, side):
        return jnp.concatenate(
            [rbuf[m, q * 16 : (q + 1) * 16, side].reshape(512, COLS) for q in range(4)], axis=1
        )

    wait_products(0)
    right = gathered(0, 1)
    for h in range(2):
        lo = h * HALF
        left = jnp.concatenate(
            [rbuf[0, q * 16 : (q + 1) * 16, 0, lo : lo + HALF].reshape(256, COLS) for q in range(4)],
            axis=1,
        )
        tri = lax.dot_general(left, right, (((1,), (1,)), ((), ())), preferred_element_type=F32)
        for q in range(4):
            tsend[0, q * 16 : (q + 1) * 16, lo : lo + HALF, :] = (
                tri[:, q * COLS : (q + 1) * COLS].reshape(16, HALF, COLS).astype(BF16)
            )
        rows_of = pl.ds(lo, HALF)
        send_all(
            lambda n: tsend.at[0, n, rows_of, :], tbuf.at[0, me, rows_of, :],
            tssem.at[0, h], trsem.at[0, h],
        )
        pltpu.make_async_copy(
            tsend.at[0, me, rows_of, :], tbuf.at[0, me, rows_of, :], own_sem.at[2, h]
        ).start()
    for h in range(2):
        lo = h * HALF
        rows_of = pl.ds(lo, HALF)
        wait_all(tbuf.at[0, pl.ds(0, DEV - 1), rows_of, :], trsem.at[0, h])
        pltpu.make_async_copy(
            tsend.at[0, me, rows_of, :], tbuf.at[0, me, rows_of, :], own_sem.at[2, h]
        ).wait()
        pair = updated(0, h, tbuf[0, :, lo : lo + HALF, :].astype(F32))
        pair_v[h] = pair
        normed_v[h] = to_rhs(norm0(pair.astype(F32)))
        products(1, h)
        send_all(lambda n: part(sbuf.at[1], n, h), part(rbuf.at[1], me, h), ssem.at[1, h], rsem.at[1, h])
        pltpu.make_async_copy(part(sbuf.at[1], me, h), part(rbuf.at[1], me, h), own_sem.at[1, h]).start()
    for h in range(2):
        gates(1, h)

    wait_products(1)
    right = gathered(1, 1)
    tri = lax.dot_general(gathered(1, 0), right, (((0,), (0,)), ((), ())), preferred_element_type=F32)
    for q in range(4):
        tsend[1, q * 16 : (q + 1) * 16, :, :] = (
            tri[:, q * COLS : (q + 1) * COLS].reshape(16, ROWS, COLS).astype(BF16)
        )
    for h in range(2):
        rows_of = pl.ds(h * HALF, HALF)
        send_all(
            lambda n: tsend.at[1, n, rows_of, :], tbuf.at[1, me, rows_of, :],
            tssem.at[1, h], trsem.at[1, h],
        )
        pltpu.make_async_copy(
            tsend.at[1, me, rows_of, :], tbuf.at[1, me, rows_of, :], own_sem.at[3, h]
        ).start()

    def across(h):
        return pltpu.make_async_remote_copy(
            src_ref=psend.at[h], dst_ref=pbuf.at[h], send_sem=pssem.at[h], recv_sem=prsem.at[h],
            device_id=(1 - tmpl, row, x), device_id_type=MESH,
        )

    for h in range(2):
        lo = h * HALF
        rows_of = pl.ds(lo, HALF)
        wait_all(tbuf.at[1, pl.ds(0, DEV - 1), rows_of, :], trsem.at[1, h])
        pltpu.make_async_copy(
            tsend.at[1, me, rows_of, :], tbuf.at[1, me, rows_of, :], own_sem.at[3, h]
        ).wait()
        pair = updated(1, h, tbuf[1, :, lo : lo + HALF, :].astype(F32))
        pooled = mask[lo : lo + HALF][None] * norm0(pair.astype(F32))
        psend[h] = pooled.astype(BF16)
        across(h).start()
    for h in range(2):
        lo = h * HALF
        across(h).wait_recv()
        pooled = psend[h].astype(F32) + pbuf[h].astype(F32)
        hidden = jnp.maximum(pooled / count[lo : lo + HALF][None], 0.0)
        out = dot(k_final[...], to_rhs(hidden))
        for side in range(2):
            first = lo + 8 * side
            block = out[:, side * COLS : (side + 1) * COLS].reshape(8, CZ, COLS)
            out_v[first : first + 8] = (tr_v[first : first + 8].astype(F32) + block).astype(BF16)
        pltpu.make_async_copy(out_v.at[rows_of_h(h)], out_hbm.at[rows_of_h(h)], st_sem.at[h]).start()

    for h in range(2):
        across(h).wait_send()
        for m in range(2):
            view = sbuf.at[m, pl.ds(0, DEV - 1), :, pl.ds(h * HALF, HALF), :]
            wait_all(view, ssem.at[m, h])
            wait_all(tsend.at[m, pl.ds(0, DEV - 1), pl.ds(h * HALF, HALF), :], tssem.at[m, h])
        pltpu.make_async_copy(out_v.at[rows_of_h(h)], out_hbm.at[rows_of_h(h)], st_sem.at[h]).wait()


def rows_of_h(h):
    return pl.ds(h * HALF, HALF)


def per_device(tp, trunk, coverage, chain_ids, chain_vec, wt, wp, wo, wf):
    vmem = pl.BlockSpec(memory_space=pltpu.VMEM)
    hbm = pl.BlockSpec(memory_space=pl.ANY)
    scratch = [
        pltpu.VMEM((ROWS, C, COLS), BF16),
        pltpu.VMEM((ROWS, CZ, COLS), BF16),
        pltpu.VMEM((ROWS, CZ, COLS), BF16),
        pltpu.VMEM((512, 512), BF16),
        pltpu.VMEM((512, 8 * CZ), BF16),
        pltpu.VMEM((2, 5, 512, 512), BF16),
        pltpu.VMEM((2, 512, 512), BF16),
        pltpu.VMEM((8 * CZ, 512), BF16),
        pltpu.VMEM((2, C, HALF, COLS), BF16),
        pltpu.VMEM((2, 512, 256), BF16),
        pltpu.VMEM((2, C, HALF, COLS), F32),
        pltpu.VMEM((2, DEV, 2, ROWS, COLS), BF16),
        pltpu.VMEM((2, DEV, 2, ROWS, COLS), BF16),
        pltpu.VMEM((2, DEV, ROWS, COLS), BF16),
        pltpu.VMEM((2, DEV, ROWS, COLS), BF16),
        pltpu.VMEM((2, C, HALF, COLS), BF16),
        pltpu.VMEM((2, C, HALF, COLS), BF16),
        pltpu.SemaphoreType.DMA((2,)),
        pltpu.SemaphoreType.DMA((2,)),
        pltpu.SemaphoreType.DMA((4, 2)),
        pltpu.SemaphoreType.DMA((2, 2)),
        pltpu.SemaphoreType.DMA((2, 2)),
        pltpu.SemaphoreType.DMA((2, 2)),
        pltpu.SemaphoreType.DMA((2, 2)),
        pltpu.SemaphoreType.DMA((2,)),
        pltpu.SemaphoreType.DMA((2,)),
    ]
    return pl.pallas_call(
        kernel,
        out_shape=jax.ShapeDtypeStruct(trunk.shape, BF16),
        in_specs=[hbm, hbm] + [vmem] * 7,
        out_specs=hbm,
        scratch_shapes=scratch,
        compiler_params=pltpu.CompilerParams(
            collective_id=0, has_side_effects=True, vmem_limit_bytes=60 * 1024 * 1024
        ),
        name="template_block",
    )(
        tp, trunk, coverage, chain_ids.reshape(1, 512), chain_vec.reshape(C, 1, 1),
        wt, wp, wo, wf,
    )


def solution(mesh):
    in_specs = (
        P("tmpl", "row", None, "col"), P("row", None, "col"),
        P(), P(), P(), P(), P(), P(), P(),
    )
    return jax.shard_map(
        per_device, mesh=mesh, in_specs=in_specs, out_specs=P("row", None, "col"), check_vma=False
    )
```

```python
import functools

import jax
import jax.numpy as jnp
from jax import lax
from jax.experimental import pallas as pl
from jax.experimental.pallas import tpu as pltpu
from jax.sharding import PartitionSpec as P

MESH = pl.DeviceIdType.MESH
EPS = 1e-05
F32 = jnp.float32
BF16 = jnp.bfloat16
ROWS, COLS, C, CZ = 32, 128, 64, 128
HALF = 16
DEV = 64


def dot(a, b):
    return jnp.dot(a, b, preferred_element_type=F32)


def iota(shape, dim):
    return lax.broadcasted_iota(jnp.int32, shape, dim)


def to_rhs(x):
    a = x[:, 0:8].reshape(512, COLS).astype(BF16)
    b = x[:, 8:16].reshape(512, COLS).astype(BF16)
    return jnp.concatenate([a, b], axis=1)


def from_out(o):
    a = o[:, 0:COLS].reshape(C, 8, COLS)
    b = o[:, COLS:].reshape(C, 8, COLS)
    return jnp.concatenate([a, b], axis=1)


def norm0(x):
    centred = x - jnp.mean(x, axis=0, keepdims=True)
    spread = jnp.mean(centred * centred, axis=0, keepdims=True)
    return centred * lax.rsqrt(spread + EPS)


def sigmoid(x):
    return 0.5 * jnp.tanh(0.5 * x) + 0.5


def kron_rows():
    return ((iota((512, C), 0) >> 3) == iota((512, C), 1)).astype(BF16)


def kron_cols():
    return ((iota((C, 512), 1) >> 3) == iota((C, 512), 0)).astype(BF16)


def kernel(
    tp_hbm, trunk_hbm, cover_ref, chain_ref, vec_ref, wt_ref, wp_ref, wo_ref, wf_ref,
    out_v,
    tp_v, tr_v, vec_v, diag_v, k_perm, k_trunk, k_proj, k_out, k_final,
    pair_v, normed_v, gate_v, tri_v, sbuf, rbuf, tsend, tbuf, psend, pbuf,
    ld_sem, own_sem, ssem, rsem, tssem, trsem, pssem, prsem,
):
    tmpl = lax.axis_index("tmpl")
    row = lax.axis_index("row")
    x = lax.axis_index("col")
    y, z = lax.div(row, 4), lax.rem(row, 4)
    me = x * 16 + row

    load_tp = pltpu.make_async_copy(tp_hbm.at[0], tp_v, ld_sem.at[0])
    load_tr = pltpu.make_async_copy(trunk_hbm, tr_v, ld_sem.at[1])
    load_tp.start()
    load_tr.start()

    peer_cols = [lax.rem(x + step, 4) for step in range(4)]

    def peer_row(step):
        mixed = lax.rem(step * 7, 16)
        return lax.rem(y + lax.div(mixed, 4), 4) * 4 + lax.rem(z + lax.rem(mixed, 4), 4)

    def each_peer(act):
        def rows_step(step, carry):
            prow = peer_row(step)
            for far in (2, 1, 3, 0):
                act(prow, peer_cols[far], peer_cols[far] * 16 + prow)
            return carry

        lax.fori_loop(1, 16, rows_step, 0)
        for far in (2, 1, 3):
            act(row, peer_cols[far], peer_cols[far] * 16 + row)

    barrier = pltpu.get_barrier_semaphore()

    def greet(prow, pcol, number):
        pl.semaphore_signal(
            barrier, inc=1, device_id=(tmpl, prow, pcol), device_id_type=MESH
        )

    each_peer(greet)
    pl.semaphore_signal(barrier, inc=1, device_id=(1 - tmpl, row, x), device_id_type=MESH)

    def send_all(source, target, send_sem, recv_sem, keep_sem):
        def send(prow, pcol, number):
            pltpu.make_async_remote_copy(
                src_ref=source(number), dst_ref=target, send_sem=send_sem, recv_sem=recv_sem,
                device_id=(tmpl, prow, pcol), device_id_type=MESH,
            ).start()

        each_peer(send)
        pltpu.make_async_copy(source(me), target, keep_sem).start()

    def wait_all(view, sem):
        pltpu.make_async_copy(view, view, sem).wait()

    def half(h):
        return pl.ds(h * HALF, HALF)

    def one_side(ref, number, side, h):
        return ref.at[0, number, side, half(h), :]

    def both_sides(ref, number, h):
        return ref.at[1, number, :, half(h), :]

    cover = cover_ref[...].astype(F32)
    picks = (iota((ROWS, 512), 1) == row * ROWS + iota((ROWS, 512), 0)).astype(BF16)

    def row_plane(line):
        spread = jnp.broadcast_to(line, (COLS, 512)).astype(BF16)
        return lax.dot_general(picks, spread, (((1,), (1,)), ((), ())), preferred_element_type=F32)

    lanes = pl.ds(pl.multiple_of(x * COLS, COLS), COLS)
    cols_of = cover_ref[:, lanes].astype(F32)
    masks = [row_plane(cover[t : t + 1]) * cols_of[t : t + 1] for t in range(2)]
    mask = jnp.where(tmpl == 0, masks[0], masks[1])
    count = jnp.maximum(masks[0] + masks[1], 1.0)
    chain_rows = row_plane(chain_ref[...].astype(F32))
    same_chain = jnp.where(chain_rows == chain_ref[:, lanes].astype(F32), 1.0, 0.0)

    for c in range(C):
        vec_v[c] = jnp.full((1, COLS), vec_ref[c], F32)
    tall_trunk = dot(kron_rows(), wt_ref[...])
    own_row = iota((512, CZ), 0) & 7
    for i in range(8):
        k_trunk[:, i * CZ : (i + 1) * CZ] = jnp.where(own_row == i, tall_trunk, 0.0).astype(BF16)
    left_row, left_col = iota((512, 512), 0), iota((512, 512), 1)
    k_perm[...] = jnp.where(
        (((left_row & 7) << 6) + (left_row >> 3)) == left_col, 1.0, 0.0
    ).astype(BF16)
    diag_v[...] = jnp.where((left_row & 7) == (left_col & 7), 1.0, 0.0)

    def kron8(w):
        tall = dot(kron_rows(), w).astype(BF16)
        return (dot(tall, kron_cols()) * diag_v[...]).astype(BF16)

    def product(m, side, h):
        rhs = normed_v[h]
        gate = from_out(dot(k_proj[m, 2 * side], rhs))
        value = from_out(dot(k_proj[m, 2 * side + 1], rhs))
        plane = mask[h * HALF : (h + 1) * HALF][None]
        sbuf[m, :, side, h * HALF : (h + 1) * HALF, :] = (plane * sigmoid(gate) * value).astype(BF16)

    def gates(m, h):
        gate_v[h] = sigmoid(from_out(dot(k_proj[m, 4], normed_v[h])))

    def updated(m, h, tri):
        tri_norm = to_rhs(norm0(tri))
        update = gate_v[h] * from_out(dot(k_out[m], tri_norm))
        return (pair_v[h].astype(F32) + update).astype(BF16)

    def send_side(side, h):
        send_all(
            lambda n: one_side(sbuf, n, side, h), one_side(rbuf, me, side, h),
            ssem.at[side, h], rsem.at[side, h], own_sem.at[side, h],
        )

    def wait_side(side, h):
        wait_all(rbuf.at[0, pl.ds(0, DEV - 1), side, half(h), :], rsem.at[side, h])
        pltpu.make_async_copy(
            one_side(sbuf, me, side, h), one_side(rbuf, me, side, h), own_sem.at[side, h]
        ).wait()

    load_tp.wait()
    load_tr.wait()
    for h in range(2):
        lo = h * HALF
        tr = tr_v[lo : lo + HALF].astype(F32)
        centred = tr - jnp.mean(tr, axis=1, keepdims=True)
        spread = jnp.mean(centred * centred, axis=1, keepdims=True)
        trn = (centred * lax.rsqrt(spread + EPS)).astype(BF16)
        rhs = jnp.concatenate(
            [trn[0:8].reshape(8 * CZ, COLS), trn[8:16].reshape(8 * CZ, COLS)], axis=1
        )
        pair = from_out(dot(k_trunk[...], rhs))
        tp = tp_v[lo : lo + HALF]
        rhs = jnp.concatenate([tp[0:8].reshape(512, COLS), tp[8:16].reshape(512, COLS)], axis=1)
        pair = pair + from_out(dot(k_perm[...], rhs))
        pair = pair + same_chain[lo : lo + HALF][None] * vec_v[...]
        pair = pair.astype(BF16)
        pair_v[h] = pair
        normed_v[h] = to_rhs(norm0(pair.astype(F32)))
        if h == 0:
            for d in (2, 3):
                k_proj[0, d] = kron8(wp_ref[0, d])
        product(0, 1, h)
        if h == 0:
            pl.semaphore_wait(barrier, DEV)
        send_side(1, h)
    for d in (0, 1):
        k_proj[0, d] = kron8(wp_ref[0, d])
    for h in range(2):
        product(0, 0, h)
        send_side(0, h)

    k_proj[0, 4] = kron8(wp_ref[0, 4])
    for h in range(2):
        gates(0, h)
    k_out[0] = kron8(wo_ref[0])
    for d in range(4):
        k_proj[1, d] = kron8(wp_ref[1, d])

    def send_tri(m, h):
        send_all(
            lambda n: tsend.at[m, n, half(h), :], tbuf.at[m, me, half(h), :],
            tssem.at[m, h], trsem.at[m, h], own_sem.at[3 + m, h],
        )

    def wait_tri(m, h):
        wait_all(tbuf.at[m, pl.ds(0, DEV - 1), half(h), :], trsem.at[m, h])
        pltpu.make_async_copy(
            tsend.at[m, me, half(h), :], tbuf.at[m, me, half(h), :], own_sem.at[3 + m, h]
        ).wait()
        return tbuf[m, :, h * HALF : (h + 1) * HALF, :].astype(F32)

    for h in range(2):
        wait_side(1, h)
    right = jnp.concatenate(
        [rbuf[0, q * 16 : (q + 1) * 16, 1].reshape(512, COLS) for q in range(4)], axis=1
    )
    for h in range(2):
        lo = h * HALF
        wait_side(0, h)
        left = jnp.concatenate(
            [rbuf[0, q * 16 : (q + 1) * 16, 0, lo : lo + HALF].reshape(256, COLS) for q in range(4)],
            axis=1,
        )
        tri = lax.dot_general(left, right, (((1,), (1,)), ((), ())), preferred_element_type=F32)
        for q in range(4):
            tsend[0, q * 16 : (q + 1) * 16, lo : lo + HALF, :] = (
                tri[:, q * COLS : (q + 1) * COLS].reshape(16, HALF, COLS).astype(BF16)
            )
        send_tri(0, h)
    for h in range(2):
        pair = updated(0, h, wait_tri(0, h))
        pair_v[h] = pair
        normed_v[h] = to_rhs(norm0(pair.astype(F32)))
        product(1, 0, h)
        product(1, 1, h)
        send_all(
            lambda n: both_sides(sbuf, n, h), both_sides(rbuf, me, h),
            ssem.at[2, h], rsem.at[2, h], own_sem.at[2, h],
        )
    k_proj[1, 4] = kron8(wp_ref[1, 4])
    for h in range(2):
        gates(1, h)
    k_out[1] = kron8(wo_ref[1])
    wide = lax.dot_general(wf_ref[...], kron_cols(), (((0,), (0,)), ((), ())), preferred_element_type=F32)
    own_col = iota((CZ, 512), 1) & 7
    for i in range(8):
        k_final[i * CZ : (i + 1) * CZ, :] = jnp.where(own_col == i, wide, 0.0).astype(BF16)

    for h in range(2):
        wait_all(rbuf.at[1, pl.ds(0, DEV - 1), :, half(h), :], rsem.at[2, h])
        pltpu.make_async_copy(both_sides(sbuf, me, h), both_sides(rbuf, me, h), own_sem.at[2, h]).wait()
        left, right = [
            jnp.concatenate(
                [
                    rbuf[1, q * 16 : (q + 1) * 16, side, h * HALF : (h + 1) * HALF].reshape(256, COLS)
                    for q in range(4)
                ],
                axis=1,
            )
            for side in range(2)
        ]
        tri = lax.dot_general(left, right, (((0,), (0,)), ((), ())), preferred_element_type=F32)
        if h == 0:
            tri_v[...] = tri
        else:
            tri = tri + tri_v[...]
    for q in range(4):
        tsend[1, q * 16 : (q + 1) * 16, :, :] = (
            tri[:, q * COLS : (q + 1) * COLS].reshape(16, ROWS, COLS).astype(BF16)
        )
    for h in range(2):
        send_tri(1, h)

    def across(h):
        return pltpu.make_async_remote_copy(
            src_ref=psend.at[h], dst_ref=pbuf.at[h], send_sem=pssem.at[h], recv_sem=prsem.at[h],
            device_id=(1 - tmpl, row, x), device_id_type=MESH,
        )

    for h in range(2):
        pair = updated(1, h, wait_tri(1, h))
        pooled = mask[h * HALF : (h + 1) * HALF][None] * norm0(pair.astype(F32))
        psend[h] = pooled.astype(BF16)
        across(h).start()
    for h in range(2):
        lo = h * HALF
        across(h).wait_recv()
        pooled = psend[h].astype(F32) + pbuf[h].astype(F32)
        hidden = jnp.maximum(pooled / count[lo : lo + HALF][None], 0.0)
        out = dot(k_final[...], to_rhs(hidden))
        for side in range(2):
            first = lo + 8 * side
            block = out[:, side * COLS : (side + 1) * COLS].reshape(8, CZ, COLS)
            out_v[first : first + 8] = (tr_v[first : first + 8].astype(F32) + block).astype(BF16)

    for h in range(2):
        across(h).wait_send()
        for side in range(2):
            wait_all(sbuf.at[0, pl.ds(0, DEV - 1), side, half(h), :], ssem.at[side, h])
        wait_all(sbuf.at[1, pl.ds(0, DEV - 1), :, half(h), :], ssem.at[2, h])
        for m in range(2):
            wait_all(tsend.at[m, pl.ds(0, DEV - 1), half(h), :], tssem.at[m, h])


def per_device(tp, trunk, coverage, chain_ids, chain_vec, wt, wp, wo, wf):
    vmem = pl.BlockSpec(memory_space=pltpu.VMEM)
    hbm = pl.BlockSpec(memory_space=pl.ANY)
    scratch = [
        pltpu.VMEM((ROWS, C, COLS), BF16),
        pltpu.VMEM((ROWS, CZ, COLS), BF16),
        pltpu.VMEM((C, 1, COLS), F32),
        pltpu.VMEM((512, 512), F32),
        pltpu.VMEM((512, 512), BF16),
        pltpu.VMEM((512, 8 * CZ), BF16),
        pltpu.VMEM((2, 5, 512, 512), BF16),
        pltpu.VMEM((2, 512, 512), BF16),
        pltpu.VMEM((8 * CZ, 512), BF16),
        pltpu.VMEM((2, C, HALF, COLS), BF16),
        pltpu.VMEM((2, 512, 256), BF16),
        pltpu.VMEM((2, C, HALF, COLS), F32),
        pltpu.VMEM((512, 512), F32),
        pltpu.VMEM((2, DEV, 2, ROWS, COLS), BF16),
        pltpu.VMEM((2, DEV, 2, ROWS, COLS), BF16),
        pltpu.VMEM((2, DEV, ROWS, COLS), BF16),
        pltpu.VMEM((2, DEV, ROWS, COLS), BF16),
        pltpu.VMEM((2, C, HALF, COLS), BF16),
        pltpu.VMEM((2, C, HALF, COLS), BF16),
        pltpu.SemaphoreType.DMA((2,)),
        pltpu.SemaphoreType.DMA((5, 2)),
        pltpu.SemaphoreType.DMA((3, 2)),
        pltpu.SemaphoreType.DMA((3, 2)),
        pltpu.SemaphoreType.DMA((2, 2)),
        pltpu.SemaphoreType.DMA((2, 2)),
        pltpu.SemaphoreType.DMA((2,)),
        pltpu.SemaphoreType.DMA((2,)),
    ]
    return pl.pallas_call(
        kernel,
        out_shape=pltpu.VMEM(trunk.shape, BF16),
        in_specs=[hbm, hbm, vmem, vmem, pl.BlockSpec(memory_space=pltpu.SMEM)] + [vmem] * 4,
        out_specs=vmem,
        scratch_shapes=scratch,
        compiler_params=pltpu.CompilerParams(
            collective_id=0, has_side_effects=True, vmem_limit_bytes=60 * 1024 * 1024
        ),
        name="template_block",
    )(
        tp, trunk, coverage, chain_ids.reshape(1, 512), chain_vec, wt, wp, wo, wf.T,
    )


def solution(mesh):
    in_specs = (
        P("tmpl", "row", None, "col"), P("row", None, "col"),
        P(), P(), P(), P(), P(), P(), P(),
    )
    return jax.shard_map(
        per_device, mesh=mesh, in_specs=in_specs, out_specs=P("row", None, "col"), check_vma=False
    )
```

```python
import functools

import jax
import jax.numpy as jnp
from jax import lax
from jax.experimental import pallas as pl
from jax.experimental.pallas import tpu as pltpu
from jax.sharding import PartitionSpec as P

MESH = pl.DeviceIdType.MESH
EPS = 1e-05
F32 = jnp.float32
BF16 = jnp.bfloat16
ROWS, COLS, C, CZ = 32, 128, 64, 128
HALF = 16
DEV = 64


def dot(a, b):
    return jnp.dot(a, b, preferred_element_type=F32)


def iota(shape, dim):
    return lax.broadcasted_iota(jnp.int32, shape, dim)


def to_rhs(x):
    a = x[:, 0:8].reshape(512, COLS).astype(BF16)
    b = x[:, 8:16].reshape(512, COLS).astype(BF16)
    return jnp.concatenate([a, b], axis=1)


def from_out(o):
    a = o[:, 0:COLS].reshape(C, 8, COLS)
    b = o[:, COLS:].reshape(C, 8, COLS)
    return jnp.concatenate([a, b], axis=1)


def norm0(x):
    centred = x - jnp.mean(x, axis=0, keepdims=True)
    spread = jnp.mean(centred * centred, axis=0, keepdims=True)
    return centred * lax.rsqrt(spread + EPS)


def sigmoid(x):
    return 0.5 * jnp.tanh(0.5 * x) + 0.5


def kron_rows():
    return ((iota((512, C), 0) >> 3) == iota((512, C), 1)).astype(BF16)


def kron_cols():
    return ((iota((C, 512), 1) >> 3) == iota((C, 512), 0)).astype(BF16)


def kernel(
    tp_hbm, trunk_hbm, cover_hbm, chain_hbm, vec_hbm, wt_hbm, wp_hbm, wo_hbm, wf_hbm,
    out_v,
    cover_ref, chain_ref, vec_ref, wt_ref, wp_ref, wo_ref, wf_ref, tp_v, tr_v, vec_v, diag_v, k_perm, k_trunk, k_proj, k_out, k_final,
    pair_v, normed_v, gate_v, tri_v, sbuf, rbuf, tsend, tbuf, psend, pbuf,
    ld_sem, own_sem, ssem, rsem, tssem, trsem, pssem, prsem,
):
    tmpl = lax.axis_index("tmpl")
    row = lax.axis_index("row")
    x = lax.axis_index("col")
    y, z = lax.div(row, 4), lax.rem(row, 4)
    me = x * 16 + row

    def load(number, source, target):
        copy = pltpu.make_async_copy(source, target, ld_sem.at[number])
        copy.start()
        return copy

    peer_cols = [lax.rem(x + step, 4) for step in range(4)]

    def away(step):
        return 2 - step + 3 * lax.div(step, 2) - 2 * lax.div(step + 1, 4)

    def each_peer(act):
        def rows_step(step, carry):
            py = lax.rem(y + away(lax.div(step, 4)), 4)
            pz = lax.rem(z + away(lax.rem(step, 4)), 4)
            prow = py * 4 + pz
            for far in (2, 1, 3, 0):
                act(prow, peer_cols[far], peer_cols[far] * 16 + prow)
            return carry

        lax.fori_loop(0, 15, rows_step, 0)
        for far in (2, 1, 3):
            act(row, peer_cols[far], peer_cols[far] * 16 + row)

    barrier = pltpu.get_barrier_semaphore()

    def greet(prow, pcol, number):
        pl.semaphore_signal(
            barrier, inc=1, device_id=(tmpl, prow, pcol), device_id_type=MESH
        )

    each_peer(greet)
    pl.semaphore_signal(barrier, inc=1, device_id=(1 - tmpl, row, x), device_id_type=MESH)

    tops = pl.ds(0, HALF), pl.ds(HALF, HALF)
    small = [
        load(0, cover_hbm, cover_ref), load(1, chain_hbm, chain_ref),
        load(2, vec_hbm, vec_ref), load(3, wt_hbm, wt_ref), load(4, wp_hbm, wp_ref),
    ]
    load_tr, load_tp = [], []
    for h in range(2):
        load_tr.append(load(5 + h, trunk_hbm.at[tops[h]], tr_v.at[tops[h]]))
        load_tp.append(load(7 + h, tp_hbm.at[0, tops[h]], tp_v.at[tops[h]]))
    late = [load(9, wo_hbm, wo_ref), load(10, wf_hbm, wf_ref)]

    def send_all(source, target, send_sem, recv_sem, keep_sem):
        def send(prow, pcol, number):
            pltpu.make_async_remote_copy(
                src_ref=source(number), dst_ref=target, send_sem=send_sem, recv_sem=recv_sem,
                device_id=(tmpl, prow, pcol), device_id_type=MESH,
            ).start()

        each_peer(send)
        pltpu.make_async_copy(source(me), target, keep_sem).start()

    def wait_all(view, sem):
        pltpu.make_async_copy(view, view, sem).wait()

    def half(h):
        return pl.ds(h * HALF, HALF)

    def block(ref, m, number, side, h):
        return ref.at[m, number, side, half(h), :]

    left_row, left_col = iota((512, 512), 0), iota((512, 512), 1)
    k_perm[...] = jnp.where(
        (((left_row & 7) << 6) + (left_row >> 3)) == left_col, 1.0, 0.0
    ).astype(BF16)
    diag_v[...] = jnp.where((left_row & 7) == (left_col & 7), 1.0, 0.0)
    for copy in small:
        copy.wait()

    cover = cover_ref[...].astype(F32)
    picks = (iota((ROWS, 512), 1) == row * ROWS + iota((ROWS, 512), 0)).astype(BF16)

    def row_plane(line):
        spread = jnp.broadcast_to(line, (COLS, 512)).astype(BF16)
        return lax.dot_general(picks, spread, (((1,), (1,)), ((), ())), preferred_element_type=F32)

    lanes = pl.ds(pl.multiple_of(x * COLS, COLS), COLS)
    cols_of = cover_ref[:, lanes].astype(F32)
    masks = [row_plane(cover[t : t + 1]) * cols_of[t : t + 1] for t in range(2)]
    mask = jnp.where(tmpl == 0, masks[0], masks[1])
    count = jnp.maximum(masks[0] + masks[1], 1.0)
    chain_rows = row_plane(chain_ref[...].astype(F32))
    same_chain = jnp.where(chain_rows == chain_ref[:, lanes].astype(F32), 1.0, 0.0)

    for c in range(C):
        vec_v[c] = jnp.full((1, COLS), vec_ref[c], F32)
    tall_trunk = dot(kron_rows(), wt_ref[...])
    own_row = iota((512, CZ), 0) & 7
    for i in range(8):
        k_trunk[:, i * CZ : (i + 1) * CZ] = jnp.where(own_row == i, tall_trunk, 0.0).astype(BF16)
    def kron8(w):
        tall = dot(kron_rows(), w).astype(BF16)
        return (dot(tall, kron_cols()) * diag_v[...]).astype(BF16)

    def product(m, side, h):
        rhs = normed_v[h]
        gate = from_out(dot(k_proj[m, 2 * side], rhs))
        value = from_out(dot(k_proj[m, 2 * side + 1], rhs))
        plane = mask[h * HALF : (h + 1) * HALF][None]
        sbuf[m, :, side, h * HALF : (h + 1) * HALF, :] = (plane * sigmoid(gate) * value).astype(BF16)

    def gates(m, h):
        gate_v[h] = sigmoid(from_out(dot(k_proj[m, 4], normed_v[h])))

    def updated(m, h, tri):
        tri_norm = to_rhs(norm0(tri))
        update = gate_v[h] * from_out(dot(k_out[m], tri_norm))
        return (pair_v[h].astype(F32) + update).astype(BF16)

    def send_side(m, side, h):
        send_all(
            lambda n: block(sbuf, m, n, side, h), block(rbuf, m, me, side, h),
            ssem.at[m, side, h], rsem.at[m, side, h], own_sem.at[m, side, h],
        )

    def wait_side(m, side, h):
        wait_all(rbuf.at[m, pl.ds(0, DEV - 1), side, half(h), :], rsem.at[m, side, h])
        pltpu.make_async_copy(
            block(sbuf, m, me, side, h), block(rbuf, m, me, side, h), own_sem.at[m, side, h]
        ).wait()

    for d in (2, 3):
        k_proj[0, d] = kron8(wp_ref[0, d])
    for h in range(2):
        lo = h * HALF
        load_tr[h].wait()
        load_tp[h].wait()
        tr = tr_v[lo : lo + HALF].astype(F32)
        centred = tr - jnp.mean(tr, axis=1, keepdims=True)
        spread = jnp.mean(centred * centred, axis=1, keepdims=True)
        trn = (centred * lax.rsqrt(spread + EPS)).astype(BF16)
        rhs = jnp.concatenate(
            [trn[0:8].reshape(8 * CZ, COLS), trn[8:16].reshape(8 * CZ, COLS)], axis=1
        )
        pair = from_out(dot(k_trunk[...], rhs))
        tp = tp_v[lo : lo + HALF]
        rhs = jnp.concatenate([tp[0:8].reshape(512, COLS), tp[8:16].reshape(512, COLS)], axis=1)
        pair = pair + from_out(dot(k_perm[...], rhs))
        pair = pair + same_chain[lo : lo + HALF][None] * vec_v[...]
        pair = pair.astype(BF16)
        pair_v[h] = pair
        normed_v[h] = to_rhs(norm0(pair.astype(F32)))
        product(0, 1, h)
        if h == 0:
            pl.semaphore_wait(barrier, DEV)
        send_side(0, 1, h)
    for d in (0, 1):
        k_proj[0, d] = kron8(wp_ref[0, d])
    for h in range(2):
        product(0, 0, h)
        send_side(0, 0, h)


    k_proj[0, 4] = kron8(wp_ref[0, 4])
    for h in range(2):
        gates(0, h)
    for copy in late:
        copy.wait()
    k_out[0] = kron8(wo_ref[0])
    for d in range(4):
        k_proj[1, d] = kron8(wp_ref[1, d])

    def send_tri(m, h):
        send_all(
            lambda n: tsend.at[m, n, half(h), :], tbuf.at[m, me, half(h), :],
            tssem.at[m, h], trsem.at[m, h], own_sem.at[2, m, h],
        )

    def wait_tri(m, h):
        wait_all(tbuf.at[m, pl.ds(0, DEV - 1), half(h), :], trsem.at[m, h])
        pltpu.make_async_copy(
            tsend.at[m, me, half(h), :], tbuf.at[m, me, half(h), :], own_sem.at[2, m, h]
        ).wait()
        return tbuf[m, :, h * HALF : (h + 1) * HALF, :].astype(F32)

    for h in range(2):
        wait_side(0, 1, h)
    right = jnp.concatenate(
        [rbuf[0, q * 16 : (q + 1) * 16, 1].reshape(512, COLS) for q in range(4)], axis=1
    )
    for h in range(2):
        lo = h * HALF
        wait_side(0, 0, h)
        left = jnp.concatenate(
            [rbuf[0, q * 16 : (q + 1) * 16, 0, lo : lo + HALF].reshape(256, COLS) for q in range(4)],
            axis=1,
        )
        tri = lax.dot_general(left, right, (((1,), (1,)), ((), ())), preferred_element_type=F32)
        for q in range(4):
            tsend[0, q * 16 : (q + 1) * 16, lo : lo + HALF, :] = (
                tri[:, q * COLS : (q + 1) * COLS].reshape(16, HALF, COLS).astype(BF16)
            )
        send_tri(0, h)
    for h in range(2):
        pair = updated(0, h, wait_tri(0, h))
        pair_v[h] = pair
        normed_v[h] = to_rhs(norm0(pair.astype(F32)))
        for side in (1, 0):
            product(1, side, h)
            send_side(1, side, h)
    k_proj[1, 4] = kron8(wp_ref[1, 4])
    for h in range(2):
        gates(1, h)
    k_out[1] = kron8(wo_ref[1])
    wide = lax.dot_general(wf_ref[...], kron_cols(), (((0,), (0,)), ((), ())), preferred_element_type=F32)
    own_col = iota((CZ, 512), 1) & 7
    for i in range(8):
        k_final[i * CZ : (i + 1) * CZ, :] = jnp.where(own_col == i, wide, 0.0).astype(BF16)

    for h in range(2):
        for side in (1, 0):
            wait_side(1, side, h)
        left, right = [
            jnp.concatenate(
                [
                    rbuf[1, q * 16 : (q + 1) * 16, side, h * HALF : (h + 1) * HALF].reshape(256, COLS)
                    for q in range(4)
                ],
                axis=1,
            )
            for side in range(2)
        ]
        tri = lax.dot_general(left, right, (((0,), (0,)), ((), ())), preferred_element_type=F32)
        if h == 0:
            tri_v[...] = tri
        else:
            tri = tri + tri_v[...]
    for q in range(4):
        tsend[1, q * 16 : (q + 1) * 16, :, :] = (
            tri[:, q * COLS : (q + 1) * COLS].reshape(16, ROWS, COLS).astype(BF16)
        )
    for h in range(2):
        send_tri(1, h)

    def across(h):
        return pltpu.make_async_remote_copy(
            src_ref=psend.at[h], dst_ref=pbuf.at[h], send_sem=pssem.at[h], recv_sem=prsem.at[h],
            device_id=(1 - tmpl, row, x), device_id_type=MESH,
        )

    for h in range(2):
        pair = updated(1, h, wait_tri(1, h))
        pooled = mask[h * HALF : (h + 1) * HALF][None] * norm0(pair.astype(F32))
        psend[h] = pooled.astype(BF16)
        across(h).start()
        across(h).wait_recv()
        lo = h * HALF
        total = psend[h].astype(F32) + pbuf[h].astype(F32)
        hidden = jnp.maximum(total / count[lo : lo + HALF][None], 0.0)
        out = dot(k_final[...], to_rhs(hidden))
        for side in range(2):
            first = lo + 8 * side
            added = out[:, side * COLS : (side + 1) * COLS].reshape(8, CZ, COLS)
            out_v[first : first + 8] = (tr_v[first : first + 8].astype(F32) + added).astype(BF16)

    for h in range(2):
        across(h).wait_send()
        for m in range(2):
            for side in range(2):
                wait_all(sbuf.at[m, pl.ds(0, DEV - 1), side, half(h), :], ssem.at[m, side, h])
            wait_all(tsend.at[m, pl.ds(0, DEV - 1), half(h), :], tssem.at[m, h])


def per_device(tp, trunk, coverage, chain_ids, chain_vec, wt, wp, wo, wf):
    vmem = pl.BlockSpec(memory_space=pltpu.VMEM)
    hbm = pl.BlockSpec(memory_space=pl.ANY)
    scratch = [
        pltpu.VMEM((2, 512), jnp.int32),
        pltpu.VMEM((1, 512), jnp.int32),
        pltpu.SMEM((C,), F32),
        pltpu.VMEM((C, CZ), BF16),
        pltpu.VMEM((2, 5, C, C), BF16),
        pltpu.VMEM((2, C, C), BF16),
        pltpu.VMEM((C, CZ), BF16),
        pltpu.VMEM((ROWS, C, COLS), BF16),
        pltpu.VMEM((ROWS, CZ, COLS), BF16),
        pltpu.VMEM((C, 1, COLS), F32),
        pltpu.VMEM((512, 512), F32),
        pltpu.VMEM((512, 512), BF16),
        pltpu.VMEM((512, 8 * CZ), BF16),
        pltpu.VMEM((2, 5, 512, 512), BF16),
        pltpu.VMEM((2, 512, 512), BF16),
        pltpu.VMEM((8 * CZ, 512), BF16),
        pltpu.VMEM((2, C, HALF, COLS), BF16),
        pltpu.VMEM((2, 512, 256), BF16),
        pltpu.VMEM((2, C, HALF, COLS), F32),
        pltpu.VMEM((512, 512), F32),
        pltpu.VMEM((2, DEV, 2, ROWS, COLS), BF16),
        pltpu.VMEM((2, DEV, 2, ROWS, COLS), BF16),
        pltpu.VMEM((2, DEV, ROWS, COLS), BF16),
        pltpu.VMEM((2, DEV, ROWS, COLS), BF16),
        pltpu.VMEM((2, C, HALF, COLS), BF16),
        pltpu.VMEM((2, C, HALF, COLS), BF16),
        pltpu.SemaphoreType.DMA((11,)),
        pltpu.SemaphoreType.DMA((3, 2, 2)),
        pltpu.SemaphoreType.DMA((2, 2, 2)),
        pltpu.SemaphoreType.DMA((2, 2, 2)),
        pltpu.SemaphoreType.DMA((2, 2)),
        pltpu.SemaphoreType.DMA((2, 2)),
        pltpu.SemaphoreType.DMA((2,)),
        pltpu.SemaphoreType.DMA((2,)),
    ]
    return pl.pallas_call(
        kernel,
        out_shape=pltpu.VMEM(trunk.shape, BF16),
        in_specs=[hbm] * 9,
        out_specs=vmem,
        scratch_shapes=scratch,
        compiler_params=pltpu.CompilerParams(
            collective_id=0, has_side_effects=True, vmem_limit_bytes=60 * 1024 * 1024
        ),
        name="template_block",
    )(
        tp, trunk, coverage, chain_ids.reshape(1, 512), chain_vec, wt, wp, wo, wf.T,
    )


def solution(mesh):
    in_specs = (
        P("tmpl", "row", None, "col"), P("row", None, "col"),
        P(), P(), P(), P(), P(), P(), P(),
    )
    return jax.shard_map(
        per_device, mesh=mesh, in_specs=in_specs, out_specs=P("row", None, "col"), check_vma=False
    )
```

```python
import functools

import jax
import jax.numpy as jnp
from jax import lax
from jax.experimental import pallas as pl
from jax.experimental.pallas import tpu as pltpu
from jax.sharding import PartitionSpec as P

MESH = pl.DeviceIdType.MESH
EPS = 1e-05
F32 = jnp.float32
BF16 = jnp.bfloat16
ROWS, COLS, C, CZ = 32, 128, 64, 128
HALF = 16
DEV = 64


def dot(a, b):
    return jnp.dot(a, b, preferred_element_type=F32)


def iota(shape, dim):
    return lax.broadcasted_iota(jnp.int32, shape, dim)


def to_rhs(x):
    a = x[:, 0:8].reshape(512, COLS).astype(BF16)
    b = x[:, 8:16].reshape(512, COLS).astype(BF16)
    return jnp.concatenate([a, b], axis=1)


def from_out(o):
    a = o[:, 0:COLS].reshape(C, 8, COLS)
    b = o[:, COLS:].reshape(C, 8, COLS)
    return jnp.concatenate([a, b], axis=1)


def norm0(x):
    centred = x - jnp.mean(x, axis=0, keepdims=True)
    spread = jnp.mean(centred * centred, axis=0, keepdims=True)
    return centred * lax.rsqrt(spread + EPS)


def sigmoid(x):
    return 0.5 * jnp.tanh(0.5 * x) + 0.5


def kron_rows():
    return ((iota((512, C), 0) >> 3) == iota((512, C), 1)).astype(BF16)


def kron_cols():
    return ((iota((C, 512), 1) >> 3) == iota((C, 512), 0)).astype(BF16)


def kernel(
    tp_hbm, trunk_hbm, cover_hbm, chain_hbm, vec_hbm, wt_hbm, wp_hbm, wo_hbm, wf_hbm,
    out_v,
    cover_ref, chain_ref, vec_ref, wt_ref, wp_ref, wo_ref, wf_ref, tp_v, tr_v, vec_v, diag_v, k_perm, k_trunk, k_proj, k_out, k_final, k_lane,
    pair_v, normed_v, gate_v, sbuf, rbuf, tsend, tbuf, psend, pbuf,
    ld_sem, own_sem, ssem, rsem, tssem, trsem, pssem, prsem,
):
    tmpl = lax.axis_index("tmpl")
    row = lax.axis_index("row")
    x = lax.axis_index("col")
    y, z = lax.div(row, 4), lax.rem(row, 4)
    me = x * 16 + row

    def load(number, source, target):
        copy = pltpu.make_async_copy(source, target, ld_sem.at[number])
        copy.start()
        return copy

    peer_cols = [lax.rem(x + step, 4) for step in range(4)]

    def away(step):
        return 2 - step + 3 * lax.div(step, 2) - 2 * lax.div(step + 1, 4)

    def each_peer(act):
        def rows_step(step, carry):
            py = lax.rem(y + away(lax.div(step, 4)), 4)
            pz = lax.rem(z + away(lax.rem(step, 4)), 4)
            prow = py * 4 + pz
            for far in (2, 1, 3, 0):
                act(prow, peer_cols[far], peer_cols[far] * 16 + prow)
            return carry

        lax.fori_loop(0, 15, rows_step, 0)
        for far in (2, 1, 3):
            act(row, peer_cols[far], peer_cols[far] * 16 + row)

    barrier = pltpu.get_barrier_semaphore()

    def greet(prow, pcol, number):
        pl.semaphore_signal(
            barrier, inc=1, device_id=(tmpl, prow, pcol), device_id_type=MESH
        )

    each_peer(greet)
    pl.semaphore_signal(barrier, inc=1, device_id=(1 - tmpl, row, x), device_id_type=MESH)

    tops = pl.ds(0, HALF), pl.ds(HALF, HALF)
    small = [
        load(0, cover_hbm, cover_ref), load(1, chain_hbm, chain_ref),
        load(2, vec_hbm, vec_ref), load(3, wt_hbm, wt_ref), load(4, wp_hbm, wp_ref),
    ]
    load_tr, load_tp = [], []
    for h in range(2):
        load_tr.append(load(5 + h, trunk_hbm.at[tops[h]], tr_v.at[tops[h]]))
        load_tp.append(load(7 + h, tp_hbm.at[0, tops[h]], tp_v.at[tops[h]]))
    late = [load(9, wo_hbm, wo_ref), load(10, wf_hbm, wf_ref)]

    def send_all(source, target, send_sem, recv_sem, keep_sem):
        def send(prow, pcol, number):
            pltpu.make_async_remote_copy(
                src_ref=source(number), dst_ref=target, send_sem=send_sem, recv_sem=recv_sem,
                device_id=(tmpl, prow, pcol), device_id_type=MESH,
            ).start()

        each_peer(send)
        pltpu.make_async_copy(source(me), target, keep_sem).start()

    def wait_all(view, sem):
        pltpu.make_async_copy(view, view, sem).wait()

    def half(h):
        return pl.ds(h * HALF, HALF)

    def block(ref, m, number, side, h):
        return ref.at[m, number, side, half(h), :]

    left_row, left_col = iota((512, 512), 0), iota((512, 512), 1)
    k_perm[...] = jnp.where(
        (((left_row & 7) << 6) + (left_row >> 3)) == left_col, 1.0, 0.0
    ).astype(BF16)
    diag_v[...] = jnp.where((left_row & 7) == (left_col & 7), 1.0, 0.0)
    for copy in small:
        copy.wait()

    cover = cover_ref[...].astype(F32)
    picks = (iota((ROWS, 512), 1) == row * ROWS + iota((ROWS, 512), 0)).astype(BF16)

    def row_plane(line):
        spread = jnp.broadcast_to(line, (COLS, 512)).astype(BF16)
        return lax.dot_general(picks, spread, (((1,), (1,)), ((), ())), preferred_element_type=F32)

    lanes = pl.ds(pl.multiple_of(x * COLS, COLS), COLS)
    cols_of = cover_ref[:, lanes].astype(F32)
    masks = [row_plane(cover[t : t + 1]) * cols_of[t : t + 1] for t in range(2)]
    mask = jnp.where(tmpl == 0, masks[0], masks[1])
    count = jnp.maximum(masks[0] + masks[1], 1.0)
    chain_rows = row_plane(chain_ref[...].astype(F32))
    same_chain = jnp.where(chain_rows == chain_ref[:, lanes].astype(F32), 1.0, 0.0)

    for c in range(C):
        vec_v[c] = jnp.full((1, COLS), vec_ref[c], F32)
    tall_trunk = dot(kron_rows(), wt_ref[...])
    own_row = iota((512, CZ), 0) & 7
    for i in range(8):
        k_trunk[:, i * CZ : (i + 1) * CZ] = jnp.where(own_row == i, tall_trunk, 0.0).astype(BF16)
    def kron8(w):
        tall = dot(kron_rows(), w).astype(BF16)
        return (dot(tall, kron_cols()) * diag_v[...]).astype(BF16)

    def product(m, side, h):
        rhs = normed_v[h]
        gate = from_out(dot(k_proj[m, 2 * side], rhs))
        value = from_out(dot(k_proj[m, 2 * side + 1], rhs))
        plane = mask[h * HALF : (h + 1) * HALF][None]
        sbuf[m, :, side, h * HALF : (h + 1) * HALF, :] = (plane * sigmoid(gate) * value).astype(BF16)

    def left_by_parts(h):
        rhs = dot(normed_v[h], k_lane[h]).astype(BF16)
        gate = from_out(dot(k_proj[1, 0], rhs))
        value = from_out(dot(k_proj[1, 1], rhs))
        plane = dot(mask[h * HALF : (h + 1) * HALF].astype(BF16), k_lane[h, 0:COLS, 0:COLS])[None]
        left = (plane * sigmoid(gate) * value).astype(BF16)
        for lanes_of in range(2):
            first = (h ^ lanes_of) * HALF
            cut = slice(lanes_of * 64, lanes_of * 64 + 64)
            sbuf[1, :, 0, first : first + HALF, cut] = left[:, :, cut]

    def gates(m, h):
        gate_v[h] = sigmoid(from_out(dot(k_proj[m, 4], normed_v[h])))

    def updated(m, h, tri):
        tri_norm = to_rhs(norm0(tri))
        update = gate_v[h] * from_out(dot(k_out[m], tri_norm))
        return (pair_v[h].astype(F32) + update).astype(BF16)

    def send_side(m, side, h):
        send_all(
            lambda n: block(sbuf, m, n, side, h), block(rbuf, m, me, side, h),
            ssem.at[m, side, h], rsem.at[m, side, h], own_sem.at[m, side, h],
        )

    def wait_side(m, side, h):
        wait_all(rbuf.at[m, pl.ds(0, DEV - 1), side, half(h), :], rsem.at[m, side, h])
        pltpu.make_async_copy(
            block(sbuf, m, me, side, h), block(rbuf, m, me, side, h), own_sem.at[m, side, h]
        ).wait()

    for d in (2, 3):
        k_proj[0, d] = kron8(wp_ref[0, d])
    for h in range(2):
        lo = h * HALF
        load_tr[h].wait()
        load_tp[h].wait()
        tr = tr_v[lo : lo + HALF].astype(F32)
        centred = tr - jnp.mean(tr, axis=1, keepdims=True)
        spread = jnp.mean(centred * centred, axis=1, keepdims=True)
        trn = (centred * lax.rsqrt(spread + EPS)).astype(BF16)
        rhs = jnp.concatenate(
            [trn[0:8].reshape(8 * CZ, COLS), trn[8:16].reshape(8 * CZ, COLS)], axis=1
        )
        pair = from_out(dot(k_trunk[...], rhs))
        tp = tp_v[lo : lo + HALF]
        rhs = jnp.concatenate([tp[0:8].reshape(512, COLS), tp[8:16].reshape(512, COLS)], axis=1)
        pair = pair + from_out(dot(k_perm[...], rhs))
        pair = pair + same_chain[lo : lo + HALF][None] * vec_v[...]
        pair = pair.astype(BF16)
        pair_v[h] = pair
        normed_v[h] = to_rhs(norm0(pair.astype(F32)))
        product(0, 1, h)
        if h == 0:
            pl.semaphore_wait(barrier, DEV)
        send_side(0, 1, h)
    for d in (0, 1):
        k_proj[0, d] = kron8(wp_ref[0, d])
    for h in range(2):
        product(0, 0, h)
        send_side(0, 0, h)


    k_proj[0, 4] = kron8(wp_ref[0, 4])
    for h in range(2):
        gates(0, h)
    for copy in late:
        copy.wait()
    k_out[0] = kron8(wo_ref[0])
    for d in range(4):
        k_proj[1, d] = kron8(wp_ref[1, d])
    old, new = iota((256, 256), 0), iota((256, 256), 1)
    for h in range(2):
        half_of = ((new >> 6) & 1) ^ h
        place = (new & 15) + (((new >> 4) & 3) << 5) + (half_of << 4) + (new & COLS)
        k_lane[h] = jnp.where(old == place, 1.0, 0.0).astype(BF16)

    def send_tri(m, h):
        send_all(
            lambda n: tsend.at[m, n, half(h), :], tbuf.at[m, me, half(h), :],
            tssem.at[m, h], trsem.at[m, h], own_sem.at[2, m, h],
        )

    def wait_tri(m, h):
        wait_all(tbuf.at[m, pl.ds(0, DEV - 1), half(h), :], trsem.at[m, h])
        pltpu.make_async_copy(
            tsend.at[m, me, half(h), :], tbuf.at[m, me, half(h), :], own_sem.at[2, m, h]
        ).wait()
        return tbuf[m, :, h * HALF : (h + 1) * HALF, :].astype(F32)

    for h in range(2):
        wait_side(0, 1, h)
    right = jnp.concatenate(
        [rbuf[0, q * 16 : (q + 1) * 16, 1].reshape(512, COLS) for q in range(4)], axis=1
    )
    for h in range(2):
        lo = h * HALF
        wait_side(0, 0, h)
        left = jnp.concatenate(
            [rbuf[0, q * 16 : (q + 1) * 16, 0, lo : lo + HALF].reshape(256, COLS) for q in range(4)],
            axis=1,
        )
        tri = lax.dot_general(left, right, (((1,), (1,)), ((), ())), preferred_element_type=F32)
        for q in range(4):
            tsend[0, q * 16 : (q + 1) * 16, lo : lo + HALF, :] = (
                tri[:, q * COLS : (q + 1) * COLS].reshape(16, HALF, COLS).astype(BF16)
            )
        send_tri(0, h)
    for h in range(2):
        pair = updated(0, h, wait_tri(0, h))
        pair_v[h] = pair
        normed_v[h] = to_rhs(norm0(pair.astype(F32)))
        product(1, 1, h)
        send_side(1, 1, h)
        left_by_parts(h)
    for part in range(2):
        send_side(1, 0, part)
    k_proj[1, 4] = kron8(wp_ref[1, 4])
    for h in range(2):
        gates(1, h)
    k_out[1] = kron8(wo_ref[1])
    wide = lax.dot_general(wf_ref[...], kron_cols(), (((0,), (0,)), ((), ())), preferred_element_type=F32)
    own_col = iota((CZ, 512), 1) & 7
    for i in range(8):
        k_final[i * CZ : (i + 1) * CZ, :] = jnp.where(own_col == i, wide, 0.0).astype(BF16)

    def stacked(side, h):
        return jnp.concatenate(
            [
                rbuf[1, q * 16 : (q + 1) * 16, side, h * HALF : (h + 1) * HALF].reshape(256, COLS)
                for q in range(4)
            ],
            axis=1,
        )

    for h in range(2):
        wait_side(1, 1, h)
    rights = [stacked(1, h) for h in range(2)]
    for part in range(2):
        wait_side(1, 0, part)
        left = stacked(0, part)
        sums = [
            lax.dot_general(left, rights[h], (((0,), (0,)), ((), ())), preferred_element_type=F32)
            .reshape(4, COLS, 512)
            for h in (part, 1 - part)
        ]
        tri = (sums[0][:, 0:64] + sums[1][:, 64:COLS]).reshape(16, HALF, 512)
        for q in range(4):
            tsend[1, q * 16 : (q + 1) * 16, part * HALF : (part + 1) * HALF, :] = (
                tri[:, :, q * COLS : (q + 1) * COLS].astype(BF16)
            )
        send_tri(1, part)

    def across(h):
        return pltpu.make_async_remote_copy(
            src_ref=psend.at[h], dst_ref=pbuf.at[h], send_sem=pssem.at[h], recv_sem=prsem.at[h],
            device_id=(1 - tmpl, row, x), device_id_type=MESH,
        )

    for h in range(2):
        pair = updated(1, h, wait_tri(1, h))
        pooled = mask[h * HALF : (h + 1) * HALF][None] * norm0(pair.astype(F32))
        psend[h] = pooled.astype(BF16)
        across(h).start()
    for h in range(2):
        across(h).wait_recv()
        lo = h * HALF
        total = psend[h].astype(F32) + pbuf[h].astype(F32)
        hidden = jnp.maximum(total / count[lo : lo + HALF][None], 0.0)
        out = dot(k_final[...], to_rhs(hidden))
        for side in range(2):
            first = lo + 8 * side
            added = out[:, side * COLS : (side + 1) * COLS].reshape(8, CZ, COLS)
            out_v[first : first + 8] = (tr_v[first : first + 8].astype(F32) + added).astype(BF16)

    for h in range(2):
        across(h).wait_send()
        for m in range(2):
            for side in range(2):
                wait_all(sbuf.at[m, pl.ds(0, DEV - 1), side, half(h), :], ssem.at[m, side, h])
            wait_all(tsend.at[m, pl.ds(0, DEV - 1), half(h), :], tssem.at[m, h])


def per_device(tp, trunk, coverage, chain_ids, chain_vec, wt, wp, wo, wf):
    vmem = pl.BlockSpec(memory_space=pltpu.VMEM)
    hbm = pl.BlockSpec(memory_space=pl.ANY)
    scratch = [
        pltpu.VMEM((2, 512), jnp.int32),
        pltpu.VMEM((1, 512), jnp.int32),
        pltpu.SMEM((C,), F32),
        pltpu.VMEM((C, CZ), BF16),
        pltpu.VMEM((2, 5, C, C), BF16),
        pltpu.VMEM((2, C, C), BF16),
        pltpu.VMEM((C, CZ), BF16),
        pltpu.VMEM((ROWS, C, COLS), BF16),
        pltpu.VMEM((ROWS, CZ, COLS), BF16),
        pltpu.VMEM((C, 1, COLS), F32),
        pltpu.VMEM((512, 512), F32),
        pltpu.VMEM((512, 512), BF16),
        pltpu.VMEM((512, 8 * CZ), BF16),
        pltpu.VMEM((2, 5, 512, 512), BF16),
        pltpu.VMEM((2, 512, 512), BF16),
        pltpu.VMEM((8 * CZ, 512), BF16),
        pltpu.VMEM((2, 256, 256), BF16),
        pltpu.VMEM((2, C, HALF, COLS), BF16),
        pltpu.VMEM((2, 512, 256), BF16),
        pltpu.VMEM((2, C, HALF, COLS), F32),
        pltpu.VMEM((2, DEV, 2, ROWS, COLS), BF16),
        pltpu.VMEM((2, DEV, 2, ROWS, COLS), BF16),
        pltpu.VMEM((2, DEV, ROWS, COLS), BF16),
        pltpu.VMEM((2, DEV, ROWS, COLS), BF16),
        pltpu.VMEM((2, C, HALF, COLS), BF16),
        pltpu.VMEM((2, C, HALF, COLS), BF16),
        pltpu.SemaphoreType.DMA((11,)),
        pltpu.SemaphoreType.DMA((3, 2, 2)),
        pltpu.SemaphoreType.DMA((2, 2, 2)),
        pltpu.SemaphoreType.DMA((2, 2, 2)),
        pltpu.SemaphoreType.DMA((2, 2)),
        pltpu.SemaphoreType.DMA((2, 2)),
        pltpu.SemaphoreType.DMA((2,)),
        pltpu.SemaphoreType.DMA((2,)),
    ]
    return pl.pallas_call(
        kernel,
        out_shape=pltpu.VMEM(trunk.shape, BF16),
        in_specs=[hbm] * 9,
        out_specs=vmem,
        scratch_shapes=scratch,
        compiler_params=pltpu.CompilerParams(
            collective_id=0, has_side_effects=True, vmem_limit_bytes=60 * 1024 * 1024
        ),
        name="template_block",
    )(
        tp, trunk, coverage, chain_ids.reshape(1, 512), chain_vec, wt, wp, wo, wf.T,
    )


def solution(mesh):
    in_specs = (
        P("tmpl", "row", None, "col"), P("row", None, "col"),
        P(), P(), P(), P(), P(), P(), P(),
    )
    return jax.shard_map(
        per_device, mesh=mesh, in_specs=in_specs, out_specs=P("row", None, "col"), check_vma=False
    )
```

```python
import functools

import jax
import jax.numpy as jnp
from jax import lax
from jax.experimental import pallas as pl
from jax.experimental.pallas import tpu as pltpu
from jax.sharding import PartitionSpec as P

MESH = pl.DeviceIdType.MESH
EPS = 1e-05
F32 = jnp.float32
BF16 = jnp.bfloat16
ROWS, COLS, C, CZ = 32, 128, 64, 128
HALF = 16
DEV = 64
STEPS = (2, 1, 3, 0)
FAR_FIRST = sorted(
    [(dx, dy, dz) for dy in STEPS for dz in STEPS for dx in STEPS if dx or dy or dz],
    key=lambda step: -sum(min(part, 4 - part) for part in step),
)


def dot(a, b):
    return jnp.dot(a, b, preferred_element_type=F32)


def iota(shape, dim):
    return lax.broadcasted_iota(jnp.int32, shape, dim)


def to_rhs(x):
    a = x[:, 0:8].reshape(512, COLS).astype(BF16)
    b = x[:, 8:16].reshape(512, COLS).astype(BF16)
    return jnp.concatenate([a, b], axis=1)


def from_out(o):
    a = o[:, 0:COLS].reshape(C, 8, COLS)
    b = o[:, COLS:].reshape(C, 8, COLS)
    return jnp.concatenate([a, b], axis=1)


def norm0(x):
    centred = x - jnp.mean(x, axis=0, keepdims=True)
    spread = jnp.mean(centred * centred, axis=0, keepdims=True)
    return centred * lax.rsqrt(spread + EPS)


def sigmoid(x):
    return 0.5 * jnp.tanh(0.5 * x) + 0.5


def kron_rows():
    return ((iota((512, C), 0) >> 3) == iota((512, C), 1)).astype(BF16)


def kron_cols():
    return ((iota((C, 512), 1) >> 3) == iota((C, 512), 0)).astype(BF16)


def kernel(
    tp_hbm, trunk_hbm, cover_hbm, chain_hbm, vec_hbm, wt_hbm, wp_hbm, wo_hbm, wf_hbm,
    out_v,
    cover_ref, chain_ref, vec_ref, wt_ref, wp_ref, wo_ref, wf_ref, tp_v, tr_v, vec_v, diag_v, k_perm, k_trunk, k_proj, k_out, k_final, k_lane,
    pair_v, normed_v, gate_v, sbuf, rbuf, tsend, tbuf, psend, pbuf,
    ld_sem, own_sem, ssem, rsem, tssem, trsem, pssem, prsem,
):
    tmpl = lax.axis_index("tmpl")
    row = lax.axis_index("row")
    x = lax.axis_index("col")
    y, z = lax.div(row, 4), lax.rem(row, 4)
    me = x * 16 + row

    def load(number, source, target):
        copy = pltpu.make_async_copy(source, target, ld_sem.at[number])
        copy.start()
        return copy

    peer_cols = [lax.rem(x + step, 4) for step in range(4)]
    peer_ys = [lax.rem(y + step, 4) * 4 for step in range(4)]
    peer_zs = [lax.rem(z + step, 4) for step in range(4)]

    def each_peer(act):
        for dx, dy, dz in FAR_FIRST:
            prow = peer_ys[dy] + peer_zs[dz]
            act(prow, peer_cols[dx], peer_cols[dx] * 16 + prow)

    barrier = pltpu.get_barrier_semaphore()

    def greet(prow, pcol, number):
        pl.semaphore_signal(
            barrier, inc=1, device_id=(tmpl, prow, pcol), device_id_type=MESH
        )

    each_peer(greet)
    pl.semaphore_signal(barrier, inc=1, device_id=(1 - tmpl, row, x), device_id_type=MESH)

    tops = pl.ds(0, HALF), pl.ds(HALF, HALF)
    small = [
        load(0, cover_hbm, cover_ref), load(1, chain_hbm, chain_ref),
        load(2, vec_hbm, vec_ref), load(3, wt_hbm, wt_ref), load(4, wp_hbm, wp_ref),
    ]
    load_tr, load_tp = [], []
    for h in range(2):
        load_tr.append(load(5 + h, trunk_hbm.at[tops[h]], tr_v.at[tops[h]]))
        load_tp.append(load(7 + h, tp_hbm.at[0, tops[h]], tp_v.at[tops[h]]))
    late = [load(9, wo_hbm, wo_ref), load(10, wf_hbm, wf_ref)]

    def send_all(source, target, send_sem, recv_sem, keep_sem):
        def send(prow, pcol, number):
            pltpu.make_async_remote_copy(
                src_ref=source(number), dst_ref=target, send_sem=send_sem, recv_sem=recv_sem,
                device_id=(tmpl, prow, pcol), device_id_type=MESH,
            ).start()

        each_peer(send)
        pltpu.make_async_copy(source(me), target, keep_sem).start()

    def wait_all(view, sem):
        pltpu.make_async_copy(view, view, sem).wait()

    def half(h):
        return pl.ds(h * HALF, HALF)

    def block(ref, m, number, side, h):
        return ref.at[m, number, side, half(h), :]

    left_row, left_col = iota((512, 512), 0), iota((512, 512), 1)
    k_perm[...] = jnp.where(
        (((left_row & 7) << 6) + (left_row >> 3)) == left_col, 1.0, 0.0
    ).astype(BF16)
    diag_v[...] = jnp.where((left_row & 7) == (left_col & 7), 1.0, 0.0)
    for copy in small:
        copy.wait()

    cover = cover_ref[...].astype(F32)
    picks = (iota((ROWS, 512), 1) == row * ROWS + iota((ROWS, 512), 0)).astype(BF16)

    def row_plane(line):
        spread = jnp.broadcast_to(line, (COLS, 512)).astype(BF16)
        return lax.dot_general(picks, spread, (((1,), (1,)), ((), ())), preferred_element_type=F32)

    lanes = pl.ds(pl.multiple_of(x * COLS, COLS), COLS)
    cols_of = cover_ref[:, lanes].astype(F32)
    masks = [row_plane(cover[t : t + 1]) * cols_of[t : t + 1] for t in range(2)]
    mask = jnp.where(tmpl == 0, masks[0], masks[1])
    count = jnp.maximum(masks[0] + masks[1], 1.0)
    chain_rows = row_plane(chain_ref[...].astype(F32))
    same_chain = jnp.where(chain_rows == chain_ref[:, lanes].astype(F32), 1.0, 0.0)

    for c in range(C):
        vec_v[c] = jnp.full((1, COLS), vec_ref[c], F32)
    tall_trunk = dot(kron_rows(), wt_ref[...])
    own_row = iota((512, CZ), 0) & 7
    for i in range(8):
        k_trunk[:, i * CZ : (i + 1) * CZ] = jnp.where(own_row == i, tall_trunk, 0.0).astype(BF16)
    def kron8(w):
        tall = dot(kron_rows(), w).astype(BF16)
        return (dot(tall, kron_cols()) * diag_v[...]).astype(BF16)

    def product(m, side, h):
        rhs = normed_v[h]
        gate = from_out(dot(k_proj[m, 2 * side], rhs))
        value = from_out(dot(k_proj[m, 2 * side + 1], rhs))
        plane = mask[h * HALF : (h + 1) * HALF][None]
        sbuf[m, :, side, h * HALF : (h + 1) * HALF, :] = (plane * sigmoid(gate) * value).astype(BF16)

    def left_by_parts(h):
        rhs = dot(normed_v[h], k_lane[h]).astype(BF16)
        gate = from_out(dot(k_proj[1, 0], rhs))
        value = from_out(dot(k_proj[1, 1], rhs))
        plane = dot(mask[h * HALF : (h + 1) * HALF].astype(BF16), k_lane[h, 0:COLS, 0:COLS])[None]
        left = (plane * sigmoid(gate) * value).astype(BF16)
        for lanes_of in range(2):
            first = (h ^ lanes_of) * HALF
            cut = slice(lanes_of * 64, lanes_of * 64 + 64)
            sbuf[1, :, 0, first : first + HALF, cut] = left[:, :, cut]

    def gates(m, h):
        gate_v[h] = sigmoid(from_out(dot(k_proj[m, 4], normed_v[h])))

    def updated(m, h, tri):
        tri_norm = to_rhs(norm0(tri))
        update = gate_v[h] * from_out(dot(k_out[m], tri_norm))
        return (pair_v[h].astype(F32) + update).astype(BF16)

    def send_side(m, side, h):
        send_all(
            lambda n: block(sbuf, m, n, side, h), block(rbuf, m, me, side, h),
            ssem.at[m, side, h], rsem.at[m, side, h], own_sem.at[m, side, h],
        )

    def wait_side(m, side, h):
        wait_all(rbuf.at[m, pl.ds(0, DEV - 1), side, half(h), :], rsem.at[m, side, h])
        pltpu.make_async_copy(
            block(sbuf, m, me, side, h), block(rbuf, m, me, side, h), own_sem.at[m, side, h]
        ).wait()

    for d in (2, 3):
        k_proj[0, d] = kron8(wp_ref[0, d])
    for h in range(2):
        lo = h * HALF
        load_tr[h].wait()
        load_tp[h].wait()
        tr = tr_v[lo : lo + HALF].astype(F32)
        centred = tr - jnp.mean(tr, axis=1, keepdims=True)
        spread = jnp.mean(centred * centred, axis=1, keepdims=True)
        trn = (centred * lax.rsqrt(spread + EPS)).astype(BF16)
        rhs = jnp.concatenate(
            [trn[0:8].reshape(8 * CZ, COLS), trn[8:16].reshape(8 * CZ, COLS)], axis=1
        )
        pair = from_out(dot(k_trunk[...], rhs))
        tp = tp_v[lo : lo + HALF]
        rhs = jnp.concatenate([tp[0:8].reshape(512, COLS), tp[8:16].reshape(512, COLS)], axis=1)
        pair = pair + from_out(dot(k_perm[...], rhs))
        pair = pair + same_chain[lo : lo + HALF][None] * vec_v[...]
        pair = pair.astype(BF16)
        pair_v[h] = pair
        normed_v[h] = to_rhs(norm0(pair.astype(F32)))
        product(0, 1, h)
        if h == 0:
            pl.semaphore_wait(barrier, DEV)
        send_side(0, 1, h)
    for d in (0, 1):
        k_proj[0, d] = kron8(wp_ref[0, d])
    for h in range(2):
        product(0, 0, h)
        send_side(0, 0, h)


    k_proj[0, 4] = kron8(wp_ref[0, 4])
    for h in range(2):
        gates(0, h)
    for copy in late:
        copy.wait()
    k_out[0] = kron8(wo_ref[0])
    for d in range(4):
        k_proj[1, d] = kron8(wp_ref[1, d])
    old, new = iota((256, 256), 0), iota((256, 256), 1)
    for h in range(2):
        half_of = ((new >> 6) & 1) ^ h
        place = (new & 15) + (((new >> 4) & 3) << 5) + (half_of << 4) + (new & COLS)
        k_lane[h] = jnp.where(old == place, 1.0, 0.0).astype(BF16)

    def send_tri(m, h):
        send_all(
            lambda n: tsend.at[m, n, half(h), :], tbuf.at[m, me, half(h), :],
            tssem.at[m, h], trsem.at[m, h], own_sem.at[2, m, h],
        )

    def wait_tri(m, h):
        wait_all(tbuf.at[m, pl.ds(0, DEV - 1), half(h), :], trsem.at[m, h])
        pltpu.make_async_copy(
            tsend.at[m, me, half(h), :], tbuf.at[m, me, half(h), :], own_sem.at[2, m, h]
        ).wait()
        return tbuf[m, :, h * HALF : (h + 1) * HALF, :].astype(F32)

    for h in range(2):
        wait_side(0, 1, h)
    right = jnp.concatenate(
        [rbuf[0, q * 16 : (q + 1) * 16, 1].reshape(512, COLS) for q in range(4)], axis=1
    )
    for h in range(2):
        lo = h * HALF
        wait_side(0, 0, h)
        left = jnp.concatenate(
            [rbuf[0, q * 16 : (q + 1) * 16, 0, lo : lo + HALF].reshape(256, COLS) for q in range(4)],
            axis=1,
        )
        tri = lax.dot_general(left, right, (((1,), (1,)), ((), ())), preferred_element_type=F32)
        for q in range(4):
            tsend[0, q * 16 : (q + 1) * 16, lo : lo + HALF, :] = (
                tri[:, q * COLS : (q + 1) * COLS].reshape(16, HALF, COLS).astype(BF16)
            )
        send_tri(0, h)
    for h in range(2):
        pair = updated(0, h, wait_tri(0, h))
        pair_v[h] = pair
        normed_v[h] = to_rhs(norm0(pair.astype(F32)))
        product(1, 1, h)
        send_side(1, 1, h)
        left_by_parts(h)
    for part in range(2):
        send_side(1, 0, part)
    k_proj[1, 4] = kron8(wp_ref[1, 4])
    for h in range(2):
        gates(1, h)
    k_out[1] = kron8(wo_ref[1])
    wide = lax.dot_general(wf_ref[...], kron_cols(), (((0,), (0,)), ((), ())), preferred_element_type=F32)
    own_col = iota((CZ, 512), 1) & 7
    for i in range(8):
        k_final[i * CZ : (i + 1) * CZ, :] = jnp.where(own_col == i, wide, 0.0).astype(BF16)

    def stacked(side, h):
        return jnp.concatenate(
            [
                rbuf[1, q * 16 : (q + 1) * 16, side, h * HALF : (h + 1) * HALF].reshape(256, COLS)
                for q in range(4)
            ],
            axis=1,
        )

    for h in range(2):
        wait_side(1, 1, h)
    rights = [stacked(1, h) for h in range(2)]
    for part in range(2):
        wait_side(1, 0, part)
        left = stacked(0, part)
        sums = [
            lax.dot_general(left, rights[h], (((0,), (0,)), ((), ())), preferred_element_type=F32)
            .reshape(4, COLS, 512)
            for h in (part, 1 - part)
        ]
        tri = (sums[0][:, 0:64] + sums[1][:, 64:COLS]).reshape(16, HALF, 512)
        for q in range(4):
            tsend[1, q * 16 : (q + 1) * 16, part * HALF : (part + 1) * HALF, :] = (
                tri[:, :, q * COLS : (q + 1) * COLS].astype(BF16)
            )
        send_tri(1, part)

    def across(h):
        return pltpu.make_async_remote_copy(
            src_ref=psend.at[h], dst_ref=pbuf.at[h], send_sem=pssem.at[h], recv_sem=prsem.at[h],
            device_id=(1 - tmpl, row, x), device_id_type=MESH,
        )

    for h in range(2):
        pair = updated(1, h, wait_tri(1, h))
        pooled = mask[h * HALF : (h + 1) * HALF][None] * norm0(pair.astype(F32))
        psend[h] = pooled.astype(BF16)
        across(h).start()
    for h in range(2):
        across(h).wait_recv()
        lo = h * HALF
        total = psend[h].astype(F32) + pbuf[h].astype(F32)
        hidden = jnp.maximum(total / count[lo : lo + HALF][None], 0.0)
        out = dot(k_final[...], to_rhs(hidden))
        for side in range(2):
            first = lo + 8 * side
            added = out[:, side * COLS : (side + 1) * COLS].reshape(8, CZ, COLS)
            out_v[first : first + 8] = (tr_v[first : first + 8].astype(F32) + added).astype(BF16)

    for h in range(2):
        across(h).wait_send()
        for m in range(2):
            for side in range(2):
                wait_all(sbuf.at[m, pl.ds(0, DEV - 1), side, half(h), :], ssem.at[m, side, h])
            wait_all(tsend.at[m, pl.ds(0, DEV - 1), half(h), :], tssem.at[m, h])


def per_device(tp, trunk, coverage, chain_ids, chain_vec, wt, wp, wo, wf):
    vmem = pl.BlockSpec(memory_space=pltpu.VMEM)
    hbm = pl.BlockSpec(memory_space=pl.ANY)
    scratch = [
        pltpu.VMEM((2, 512), jnp.int32),
        pltpu.VMEM((1, 512), jnp.int32),
        pltpu.SMEM((C,), F32),
        pltpu.VMEM((C, CZ), BF16),
        pltpu.VMEM((2, 5, C, C), BF16),
        pltpu.VMEM((2, C, C), BF16),
        pltpu.VMEM((C, CZ), BF16),
        pltpu.VMEM((ROWS, C, COLS), BF16),
        pltpu.VMEM((ROWS, CZ, COLS), BF16),
        pltpu.VMEM((C, 1, COLS), F32),
        pltpu.VMEM((512, 512), F32),
        pltpu.VMEM((512, 512), BF16),
        pltpu.VMEM((512, 8 * CZ), BF16),
        pltpu.VMEM((2, 5, 512, 512), BF16),
        pltpu.VMEM((2, 512, 512), BF16),
        pltpu.VMEM((8 * CZ, 512), BF16),
        pltpu.VMEM((2, 256, 256), BF16),
        pltpu.VMEM((2, C, HALF, COLS), BF16),
        pltpu.VMEM((2, 512, 256), BF16),
        pltpu.VMEM((2, C, HALF, COLS), F32),
        pltpu.VMEM((2, DEV, 2, ROWS, COLS), BF16),
        pltpu.VMEM((2, DEV, 2, ROWS, COLS), BF16),
        pltpu.VMEM((2, DEV, ROWS, COLS), BF16),
        pltpu.VMEM((2, DEV, ROWS, COLS), BF16),
        pltpu.VMEM((2, C, HALF, COLS), BF16),
        pltpu.VMEM((2, C, HALF, COLS), BF16),
        pltpu.SemaphoreType.DMA((11,)),
        pltpu.SemaphoreType.DMA((3, 2, 2)),
        pltpu.SemaphoreType.DMA((2, 2, 2)),
        pltpu.SemaphoreType.DMA((2, 2, 2)),
        pltpu.SemaphoreType.DMA((2, 2)),
        pltpu.SemaphoreType.DMA((2, 2)),
        pltpu.SemaphoreType.DMA((2,)),
        pltpu.SemaphoreType.DMA((2,)),
    ]
    return pl.pallas_call(
        kernel,
        out_shape=pltpu.VMEM(trunk.shape, BF16),
        in_specs=[hbm] * 9,
        out_specs=vmem,
        scratch_shapes=scratch,
        compiler_params=pltpu.CompilerParams(
            collective_id=0, has_side_effects=True, vmem_limit_bytes=60 * 1024 * 1024
        ),
        name="template_block",
    )(
        tp, trunk, coverage, chain_ids.reshape(1, 512), chain_vec, wt, wp, wo, wf.T,
    )


def solution(mesh):
    in_specs = (
        P("tmpl", "row", None, "col"), P("row", None, "col"),
        P(), P(), P(), P(), P(), P(), P(),
    )
    return jax.shard_map(
        per_device, mesh=mesh, in_specs=in_specs, out_specs=P("row", None, "col"), check_vma=False
    )
```

```python
import functools

import jax
import jax.numpy as jnp
from jax import lax
from jax.experimental import pallas as pl
from jax.experimental.pallas import tpu as pltpu
from jax.sharding import PartitionSpec as P

MESH = pl.DeviceIdType.MESH
EPS = 1e-05
F32 = jnp.float32
BF16 = jnp.bfloat16
ROWS, COLS, C, CZ = 32, 128, 64, 128
HALF = 16
DEV = 64
STEPS = (2, 1, 3, 0)
FAR_FIRST = sorted(
    [(dx, dy, dz) for dy in STEPS for dz in STEPS for dx in STEPS if dx or dy or dz],
    key=lambda step: -sum(min(part, 4 - part) for part in step),
)


def dot(a, b):
    return jnp.dot(a, b, preferred_element_type=F32)


def iota(shape, dim):
    return lax.broadcasted_iota(jnp.int32, shape, dim)


def to_rhs(x):
    a = x[:, 0:8].reshape(512, COLS).astype(BF16)
    b = x[:, 8:16].reshape(512, COLS).astype(BF16)
    return jnp.concatenate([a, b], axis=1)


def from_out(o):
    a = o[:, 0:COLS].reshape(C, 8, COLS)
    b = o[:, COLS:].reshape(C, 8, COLS)
    return jnp.concatenate([a, b], axis=1)


def norm0(x):
    centred = x - jnp.mean(x, axis=0, keepdims=True)
    spread = jnp.mean(centred * centred, axis=0, keepdims=True)
    return centred * lax.rsqrt(spread + EPS)


def sigmoid(x):
    return 0.5 * jnp.tanh(0.5 * x) + 0.5


def kron_rows():
    return ((iota((512, C), 0) >> 3) == iota((512, C), 1)).astype(BF16)


def kron_cols():
    return ((iota((C, 512), 1) >> 3) == iota((C, 512), 0)).astype(BF16)


def kernel(
    tp_hbm, trunk_hbm, cover_hbm, chain_hbm, vec_hbm, wt_hbm, wp_hbm, wo_hbm, wf_hbm,
    out_v,
    cover_ref, chain_ref, vec_ref, wt_ref, wp_ref, wo_ref, wf_ref, tp_v, tr_v, vec_v, diag_v, k_perm, k_trunk, k_proj, k_out, k_final, k_lane,
    pair_v, normed_v, gate_v, sbuf, rbuf, tsend, tbuf, psend, pbuf,
    ld_sem, own_sem, ssem, rsem, tssem, trsem, pssem, prsem, lsem,
):
    tmpl = lax.axis_index("tmpl")
    row = lax.axis_index("row")
    x = lax.axis_index("col")
    y, z = lax.div(row, 4), lax.rem(row, 4)
    me = x * 16 + row

    def load(number, source, target):
        copy = pltpu.make_async_copy(source, target, ld_sem.at[number])
        copy.start()
        return copy

    peer_cols = [lax.rem(x + step, 4) for step in range(4)]
    peer_ys = [lax.rem(y + step, 4) * 4 for step in range(4)]
    peer_zs = [lax.rem(z + step, 4) for step in range(4)]

    def each_peer(act):
        for dx, dy, dz in FAR_FIRST:
            prow = peer_ys[dy] + peer_zs[dz]
            act(prow, peer_cols[dx], peer_cols[dx] * 16 + prow)

    barrier = pltpu.get_barrier_semaphore()

    def greet(prow, pcol, number):
        pl.semaphore_signal(
            barrier, inc=1, device_id=(tmpl, prow, pcol), device_id_type=MESH
        )

    each_peer(greet)
    pl.semaphore_signal(barrier, inc=1, device_id=(1 - tmpl, row, x), device_id_type=MESH)

    tops = pl.ds(0, HALF), pl.ds(HALF, HALF)
    small = [
        load(0, cover_hbm, cover_ref), load(1, chain_hbm, chain_ref),
        load(2, vec_hbm, vec_ref), load(3, wt_hbm, wt_ref), load(4, wp_hbm, wp_ref),
    ]
    load_tr, load_tp = [], []
    for h in range(2):
        load_tr.append(load(5 + h, trunk_hbm.at[tops[h]], tr_v.at[tops[h]]))
        load_tp.append(load(7 + h, tp_hbm.at[0, tops[h]], tp_v.at[tops[h]]))
    late = [load(9, wo_hbm, wo_ref), load(10, wf_hbm, wf_ref)]

    def send_all(source, target, send_sem, recv_sem, keep_sem):
        def send(prow, pcol, number):
            pltpu.make_async_remote_copy(
                src_ref=source(number), dst_ref=target, send_sem=send_sem, recv_sem=recv_sem,
                device_id=(tmpl, prow, pcol), device_id_type=MESH,
            ).start()

        each_peer(send)
        pltpu.make_async_copy(source(me), target, keep_sem).start()

    def wait_all(view, sem):
        pltpu.make_async_copy(view, view, sem).wait()

    def half(h):
        return pl.ds(h * HALF, HALF)

    def block(ref, m, number, side, h):
        return ref.at[m, number, side, half(h), :]

    left_row, left_col = iota((512, 512), 0), iota((512, 512), 1)
    k_perm[...] = jnp.where(
        (((left_row & 7) << 6) + (left_row >> 3)) == left_col, 1.0, 0.0
    ).astype(BF16)
    diag_v[...] = jnp.where((left_row & 7) == (left_col & 7), 1.0, 0.0)
    for copy in small:
        copy.wait()

    cover = cover_ref[...].astype(F32)
    picks = (iota((ROWS, 512), 1) == row * ROWS + iota((ROWS, 512), 0)).astype(BF16)

    def row_plane(line):
        spread = jnp.broadcast_to(line, (COLS, 512)).astype(BF16)
        return lax.dot_general(picks, spread, (((1,), (1,)), ((), ())), preferred_element_type=F32)

    lanes = pl.ds(pl.multiple_of(x * COLS, COLS), COLS)
    cols_of = cover_ref[:, lanes].astype(F32)
    masks = [row_plane(cover[t : t + 1]) * cols_of[t : t + 1] for t in range(2)]
    mask = jnp.where(tmpl == 0, masks[0], masks[1])
    share = 1.0 / jnp.maximum(masks[0] + masks[1], 1.0)
    chain_rows = row_plane(chain_ref[...].astype(F32))
    same_chain = jnp.where(chain_rows == chain_ref[:, lanes].astype(F32), 1.0, 0.0)

    for c in range(C):
        vec_v[c] = jnp.full((1, COLS), vec_ref[c], F32)
    tall_trunk = dot(kron_rows(), wt_ref[...])
    own_row = iota((512, CZ), 0) & 7
    for i in range(8):
        k_trunk[:, i * CZ : (i + 1) * CZ] = jnp.where(own_row == i, tall_trunk, 0.0).astype(BF16)
    def kron8(w):
        tall = dot(kron_rows(), w).astype(BF16)
        return (dot(tall, kron_cols()) * diag_v[...]).astype(BF16)

    def product(m, side, h):
        rhs = normed_v[h]
        gate = from_out(dot(k_proj[m, 2 * side], rhs))
        value = from_out(dot(k_proj[m, 2 * side + 1], rhs))
        plane = mask[h * HALF : (h + 1) * HALF][None]
        sbuf[m, :, side, h * HALF : (h + 1) * HALF, :] = (plane * sigmoid(gate) * value).astype(BF16)

    def left_by_parts(h):
        rhs = dot(normed_v[h], k_lane[h]).astype(BF16)
        gate = from_out(dot(k_proj[1, 0], rhs))
        value = from_out(dot(k_proj[1, 1], rhs))
        plane = dot(mask[h * HALF : (h + 1) * HALF].astype(BF16), k_lane[h, 0:COLS, 0:COLS])[None]
        left = (plane * sigmoid(gate) * value).astype(BF16)
        for lanes_of in range(2):
            first = (h ^ lanes_of) * HALF
            cut = slice(lanes_of * 64, lanes_of * 64 + 64)
            sbuf[1, :, 0, first : first + HALF, cut] = left[:, :, cut]

    def gates(m, h):
        gate_v[h] = sigmoid(from_out(dot(k_proj[m, 4], normed_v[h])))

    def updated(m, h, tri):
        tri_norm = to_rhs(norm0(tri))
        update = gate_v[h] * from_out(dot(k_out[m], tri_norm))
        return (pair_v[h].astype(F32) + update).astype(BF16)

    def eighth(ref, number, e):
        return ref.at[0, number, 0, pl.ds(e * 8, 8), :]

    def tri_rows(ref, number, e):
        return ref.at[0, number, pl.ds(e * 8, 8), :]

    def send_side(m, side, h):
        send_all(
            lambda n: block(sbuf, m, n, side, h), block(rbuf, m, me, side, h),
            ssem.at[m, side, h], rsem.at[m, side, h], own_sem.at[m, side, h],
        )

    def wait_side(m, side, h):
        wait_all(rbuf.at[m, pl.ds(0, DEV - 1), side, half(h), :], rsem.at[m, side, h])
        pltpu.make_async_copy(
            block(sbuf, m, me, side, h), block(rbuf, m, me, side, h), own_sem.at[m, side, h]
        ).wait()

    for d in (2, 3):
        k_proj[0, d] = kron8(wp_ref[0, d])
    for h in range(2):
        lo = h * HALF
        load_tr[h].wait()
        load_tp[h].wait()
        tr = tr_v[lo : lo + HALF].astype(F32)
        centred = tr - jnp.mean(tr, axis=1, keepdims=True)
        spread = jnp.mean(centred * centred, axis=1, keepdims=True)
        trn = (centred * lax.rsqrt(spread + EPS)).astype(BF16)
        rhs = jnp.concatenate(
            [trn[0:8].reshape(8 * CZ, COLS), trn[8:16].reshape(8 * CZ, COLS)], axis=1
        )
        pair = from_out(dot(k_trunk[...], rhs))
        tp = tp_v[lo : lo + HALF]
        rhs = jnp.concatenate([tp[0:8].reshape(512, COLS), tp[8:16].reshape(512, COLS)], axis=1)
        pair = pair + from_out(dot(k_perm[...], rhs))
        pair = pair + same_chain[lo : lo + HALF][None] * vec_v[...]
        pair = pair.astype(BF16)
        pair_v[h] = pair
        normed_v[h] = to_rhs(norm0(pair.astype(F32)))
        product(0, 1, h)
        if h == 0:
            pl.semaphore_wait(barrier, DEV)
        send_side(0, 1, h)
    for d in (0, 1):
        k_proj[0, d] = kron8(wp_ref[0, d])
    for h in range(2):
        product(0, 0, h)
        for e in (2 * h, 2 * h + 1):
            send_all(
                lambda n: eighth(sbuf, n, e), eighth(rbuf, me, e),
                lsem.at[0, e], lsem.at[1, e], lsem.at[2, e],
            )


    k_proj[0, 4] = kron8(wp_ref[0, 4])
    for h in range(2):
        gates(0, h)
    for copy in late:
        copy.wait()
    k_out[0] = kron8(wo_ref[0])
    for d in range(4):
        k_proj[1, d] = kron8(wp_ref[1, d])
    old, new = iota((256, 256), 0), iota((256, 256), 1)
    for h in range(2):
        half_of = ((new >> 6) & 1) ^ h
        place = (new & 15) + (((new >> 4) & 3) << 5) + (half_of << 4) + (new & COLS)
        k_lane[h] = jnp.where(old == place, 1.0, 0.0).astype(BF16)

    def send_tri(m, h):
        send_all(
            lambda n: tsend.at[m, n, half(h), :], tbuf.at[m, me, half(h), :],
            tssem.at[m, h], trsem.at[m, h], own_sem.at[2, m, h],
        )

    def wait_tri(m, h):
        wait_all(tbuf.at[m, pl.ds(0, DEV - 1), half(h), :], trsem.at[m, h])
        pltpu.make_async_copy(
            tsend.at[m, me, half(h), :], tbuf.at[m, me, half(h), :], own_sem.at[2, m, h]
        ).wait()
        return tbuf[m, :, h * HALF : (h + 1) * HALF, :].astype(F32)

    for h in range(2):
        wait_side(0, 1, h)
    right = jnp.concatenate(
        [rbuf[0, q * 16 : (q + 1) * 16, 1].reshape(512, COLS) for q in range(4)], axis=1
    )
    for e in range(4):
        lo = e * 8
        wait_all(rbuf.at[0, pl.ds(0, DEV - 1), 0, pl.ds(lo, 8), :], lsem.at[1, e])
        pltpu.make_async_copy(eighth(sbuf, me, e), eighth(rbuf, me, e), lsem.at[2, e]).wait()
        left = jnp.concatenate(
            [rbuf[0, q * 16 : (q + 1) * 16, 0, lo : lo + 8].reshape(128, COLS) for q in range(4)],
            axis=1,
        )
        tri = lax.dot_general(left, right, (((1,), (1,)), ((), ())), preferred_element_type=F32)
        for q in range(4):
            tsend[0, q * 16 : (q + 1) * 16, lo : lo + 8, :] = (
                tri[:, q * COLS : (q + 1) * COLS].reshape(16, 8, COLS).astype(BF16)
            )
        send_all(
            lambda n: tri_rows(tsend, n, e), tri_rows(tbuf, me, e),
            lsem.at[3, e], lsem.at[4, e], lsem.at[5, e],
        )
    for h in range(2):
        for e in (2 * h, 2 * h + 1):
            wait_all(tbuf.at[0, pl.ds(0, DEV - 1), pl.ds(e * 8, 8), :], lsem.at[4, e])
            pltpu.make_async_copy(tri_rows(tsend, me, e), tri_rows(tbuf, me, e), lsem.at[5, e]).wait()
        pair = updated(0, h, tbuf[0, :, h * HALF : (h + 1) * HALF, :].astype(F32))
        pair_v[h] = pair
        normed_v[h] = to_rhs(norm0(pair.astype(F32)))
        product(1, 1, h)
        send_side(1, 1, h)
        left_by_parts(h)
    for part in range(2):
        send_side(1, 0, part)
    k_proj[1, 4] = kron8(wp_ref[1, 4])
    for h in range(2):
        gates(1, h)
    k_out[1] = kron8(wo_ref[1])
    wide = lax.dot_general(wf_ref[...], kron_cols(), (((0,), (0,)), ((), ())), preferred_element_type=F32)
    own_col = iota((CZ, 512), 1) & 7
    for i in range(8):
        k_final[i * CZ : (i + 1) * CZ, :] = jnp.where(own_col == i, wide, 0.0).astype(BF16)

    def stacked(side, h):
        return jnp.concatenate(
            [
                rbuf[1, q * 16 : (q + 1) * 16, side, h * HALF : (h + 1) * HALF].reshape(256, COLS)
                for q in range(4)
            ],
            axis=1,
        )

    for h in range(2):
        wait_side(1, 1, h)
    rights = [stacked(1, h) for h in range(2)]
    for part in range(2):
        wait_side(1, 0, part)
        left = stacked(0, part)
        sums = [
            lax.dot_general(left, rights[h], (((0,), (0,)), ((), ())), preferred_element_type=F32)
            .reshape(4, COLS, 512)
            for h in (part, 1 - part)
        ]
        tri = (sums[0][:, 0:64] + sums[1][:, 64:COLS]).reshape(16, HALF, 512)
        for q in range(4):
            tsend[1, q * 16 : (q + 1) * 16, part * HALF : (part + 1) * HALF, :] = (
                tri[:, :, q * COLS : (q + 1) * COLS].astype(BF16)
            )
        send_tri(1, part)

    def across(h):
        return pltpu.make_async_remote_copy(
            src_ref=psend.at[h], dst_ref=pbuf.at[h], send_sem=pssem.at[h], recv_sem=prsem.at[h],
            device_id=(1 - tmpl, row, x), device_id_type=MESH,
        )

    for h in range(2):
        pair = updated(1, h, wait_tri(1, h))
        pooled = mask[h * HALF : (h + 1) * HALF][None] * norm0(pair.astype(F32))
        psend[h] = pooled.astype(BF16)
        across(h).start()
    for h in range(2):
        across(h).wait_recv()
        lo = h * HALF
        total = psend[h].astype(F32) + pbuf[h].astype(F32)
        hidden = jnp.maximum(total * share[lo : lo + HALF][None], 0.0)
        out = dot(k_final[...], to_rhs(hidden))
        for side in range(2):
            first = lo + 8 * side
            added = out[:, side * COLS : (side + 1) * COLS].reshape(8, CZ, COLS)
            out_v[first : first + 8] = (tr_v[first : first + 8].astype(F32) + added).astype(BF16)

    for h in range(2):
        across(h).wait_send()
        wait_all(sbuf.at[0, pl.ds(0, DEV - 1), 1, half(h), :], ssem.at[0, 1, h])
        for side in range(2):
            wait_all(sbuf.at[1, pl.ds(0, DEV - 1), side, half(h), :], ssem.at[1, side, h])
        wait_all(tsend.at[1, pl.ds(0, DEV - 1), half(h), :], tssem.at[1, h])
    for e in range(4):
        wait_all(sbuf.at[0, pl.ds(0, DEV - 1), 0, pl.ds(e * 8, 8), :], lsem.at[0, e])
        wait_all(tsend.at[0, pl.ds(0, DEV - 1), pl.ds(e * 8, 8), :], lsem.at[3, e])


def per_device(tp, trunk, coverage, chain_ids, chain_vec, wt, wp, wo, wf):
    vmem = pl.BlockSpec(memory_space=pltpu.VMEM)
    hbm = pl.BlockSpec(memory_space=pl.ANY)
    scratch = [
        pltpu.VMEM((2, 512), jnp.int32),
        pltpu.VMEM((1, 512), jnp.int32),
        pltpu.SMEM((C,), F32),
        pltpu.VMEM((C, CZ), BF16),
        pltpu.VMEM((2, 5, C, C), BF16),
        pltpu.VMEM((2, C, C), BF16),
        pltpu.VMEM((C, CZ), BF16),
        pltpu.VMEM((ROWS, C, COLS), BF16),
        pltpu.VMEM((ROWS, CZ, COLS), BF16),
        pltpu.VMEM((C, 1, COLS), F32),
        pltpu.VMEM((512, 512), F32),
        pltpu.VMEM((512, 512), BF16),
        pltpu.VMEM((512, 8 * CZ), BF16),
        pltpu.VMEM((2, 5, 512, 512), BF16),
        pltpu.VMEM((2, 512, 512), BF16),
        pltpu.VMEM((8 * CZ, 512), BF16),
        pltpu.VMEM((2, 256, 256), BF16),
        pltpu.VMEM((2, C, HALF, COLS), BF16),
        pltpu.VMEM((2, 512, 256), BF16),
        pltpu.VMEM((2, C, HALF, COLS), F32),
        pltpu.VMEM((2, DEV, 2, ROWS, COLS), BF16),
        pltpu.VMEM((2, DEV, 2, ROWS, COLS), BF16),
        pltpu.VMEM((2, DEV, ROWS, COLS), BF16),
        pltpu.VMEM((2, DEV, ROWS, COLS), BF16),
        pltpu.VMEM((2, C, HALF, COLS), BF16),
        pltpu.VMEM((2, C, HALF, COLS), BF16),
        pltpu.SemaphoreType.DMA((11,)),
        pltpu.SemaphoreType.DMA((3, 2, 2)),
        pltpu.SemaphoreType.DMA((2, 2, 2)),
        pltpu.SemaphoreType.DMA((2, 2, 2)),
        pltpu.SemaphoreType.DMA((2, 2)),
        pltpu.SemaphoreType.DMA((2, 2)),
        pltpu.SemaphoreType.DMA((2,)),
        pltpu.SemaphoreType.DMA((2,)),
        pltpu.SemaphoreType.DMA((6, 4)),
    ]
    return pl.pallas_call(
        kernel,
        out_shape=pltpu.VMEM(trunk.shape, BF16),
        in_specs=[hbm] * 9,
        out_specs=vmem,
        scratch_shapes=scratch,
        compiler_params=pltpu.CompilerParams(
            collective_id=0, has_side_effects=True, vmem_limit_bytes=60 * 1024 * 1024
        ),
        name="template_block",
    )(
        tp, trunk, coverage, chain_ids.reshape(1, 512), chain_vec, wt, wp, wo, wf.T,
    )


def solution(mesh):
    in_specs = (
        P("tmpl", "row", None, "col"), P("row", None, "col"),
        P(), P(), P(), P(), P(), P(), P(),
    )
    return jax.shard_map(
        per_device, mesh=mesh, in_specs=in_specs, out_specs=P("row", None, "col"), check_vma=False
    )
```
